128 devices in a mesh: grp: 8 (over x, core), row: 16 (over y, z).
Axes of the slice: x: 4, y: 4, z: 4, core: 2. Of those that a mesh axis runs over, the one named last changes fastest.
Arguments:
- table: float32 [16, 131072, 128], P('grp', 'row'), may hold values from -6 to 6
- row_shard: int32 [16, 32768, 1], P('grp'), may hold values from 0 to 15; in each aligned block of 256 rows (0 to 255, 256 to 511, ..., all dimensions but the last counted through in order) at most 48 rows name the same one
- row_offset: int32 [16, 32768], P('grp'), may hold values from 0 to 8191
- bag_lengths: int32 [16, 128, 128], P('grp'), may hold values from 1 to 4, 256 in all within a row
Outputs:
- pooled: float32 [16, 16384, 128], P(None, ('grp', 'row'))
The draws below stay inside these ranges and needn't reach their ends.
Inputs may be any that keep to these rules, and one draw needn't show every extreme that they name: `row_shard`: in each aligned block of 256 lookups of a table (the lookups of one block of bags), at most 48 lookups name the same row shard, and in every draw some block reaches 48. `bag_lengths`: the 128 lengths of each block sum to 256.
All inputs are finite; a program needn't handle non-finite values.
Results may differ from the reference program's by a relative error of at most 0.0003.
Values sent between devices are 32-bit elements; how exact they have to be, the bound alone decides.
No kernel may reach another device: no remote copies, remote signals or barrier semaphores. Data moves between devices by JAX's collectives and lax.ppermute only.
A program may use at most 64 MiB of HBM per device.

```python
import math
import jax
import jax.numpy as jnp
import numpy as np
from jax import lax

E = 128
POOL = 2
BAGS_BLK = 128
ROWS_DEV = 8192
TABLES = 16
BLOCKS = 128
BAGS = 16384
LOOK_BLK = 256
LOOKUPS = 32768
ROWS = 131072
CAP = 48
N_ROW = 16


def place_ends(array, key, low, high):
    place = [jax.random.randint(jax.random.fold_in(key, axis), (), 0, length) for axis, length in enumerate(array.shape)]
    main_axis = array.shape.index(max(array.shape))
    neighbour = place[:main_axis] + [(place[main_axis] + 1) % array.shape[main_axis]] + place[main_axis + 1:]
    return array.at[tuple(place)].set(low).at[tuple(neighbour)].set(high)


def block_scale(own_key, shape, cuts, smallest, high):
    def one(axis_at, parts):
        steps = jax.random.uniform(jax.random.fold_in(jax.random.fold_in(own_key, 6), axis_at), (parts,), jnp.float32, smallest / len(cuts), high / len(cuts))
        return jnp.repeat(jnp.exp(steps), shape[axis_at] // parts).reshape((-1,) + (1,) * (len(shape) - axis_at - 1))

    gain = one(*cuts[0])
    for cut in cuts[1:]:
        gain = gain * one(*cut)
    return gain


def split_up(number_of, total, bound, lean):
    weights = [(1 << 20) // math.isqrt(grade ** lean) + 1 for grade in range(2, number_of + 1)]
    rest, given = total - bound - (number_of - 1), [1] * (number_of - 1)
    while rest > 0:
        movable = [i for i in range(number_of - 1) if given[i] < bound]
        whole, left = sum([weights[i] for i in movable]), rest
        for i in movable:
            extra = min(bound - given[i], max(1, left * weights[i] // whole), rest)
            given[i] = given[i] + extra
            rest = rest - extra
    return np.array([bound] + given)


def ragged(own_key, amount, total, bound, slope):
    if amount == 2:
        one = jax.random.randint(own_key, (), max(1, total - bound), min(bound, total - 1) + 1)
        return jnp.stack([one, total - one])
    sizes = jnp.asarray(split_up(amount, total, bound, slope), jnp.int32)
    pairs = (amount - 1) // 2
    source_of, sink = sizes[1:1 + 2 * pairs:2], sizes[2:2 + 2 * pairs:2]
    margin = jnp.minimum(source_of - 1, bound - sink)
    shifted = jax.random.randint(jax.random.fold_in(own_key, 1), (pairs,), 0, 1 << 20) % (margin + 1)
    sizes = sizes.at[1:1 + 2 * pairs:2].set(source_of - shifted).at[2:2 + 2 * pairs:2].set(sink + shifted)
    return sizes[jax.random.permutation(jax.random.fold_in(own_key, 2), amount)]


def assign_block(stream_key, own, number, rows, amount, top, reach, skew):
    ranking = jax.random.permutation(stream_key, amount)
    crowded, ordinary = load_shares(amount, rows * top, reach, skew, True), load_shares(amount, rows * top, reach, skew, False)
    places = jnp.arange(amount)

    def named(sizes, offset_by):
        used = int((sizes > 0).sum())
        fixed = max(1, used // 4)
        passed = fixed + (places - fixed + offset_by * (used - fixed)) % max(1, amount - fixed)
        return jnp.zeros((amount,), jnp.int32).at[ranking[jnp.where(places < fixed, places, passed)]].set(jnp.asarray(sizes, jnp.int32))

    sizes = jnp.where(number % 4 == 0, named(crowded, number // 4), named(ordinary, number - number // 4 - 1))
    mixed = jax.random.permutation(jax.random.fold_in(own, 3), amount)
    source_of, receiver = mixed[0:amount // 2 * 2:2], mixed[1:amount // 2 * 2:2]
    slack = jnp.minimum(sizes[source_of] - 1, reach - sizes[receiver]) // 2
    slack = jnp.where((source_of == ranking[0]) | (receiver == ranking[0]) | (sizes[receiver] == 0), 0, jnp.maximum(slack, 0))
    passed = jax.random.randint(jax.random.fold_in(own, 4), (amount // 2,), 0, 1 << 20) % (slack + 1)
    sizes = sizes.at[source_of].add(-passed).at[receiver].add(passed)
    members = jnp.searchsorted(jnp.cumsum(sizes), jnp.arange(rows * top), side="right").astype(jnp.int32)
    grid = members.reshape(top, rows).T
    grid = grid[jax.random.permutation(jax.random.fold_in(own, 1), rows)]
    offset_by = jax.random.randint(jax.random.fold_in(own, 2), (rows, 1), 0, top)
    return jnp.take_along_axis(grid, (jnp.arange(top)[None, :] + offset_by) % top, axis=1)


def load_shares(count, total, reach, skew, full):
    portions = [(1 << 20) // math.isqrt(standing ** skew) + 1 for standing in range(1, count + 1)]
    largest = reach if full else min(reach, max(-(-total // count), total * portions[0] // sum(portions)))
    least = 1 if total - largest >= count - 1 else 0
    given, rest = [largest] + [least] * (count - 1), total - largest - least * (count - 1)
    while rest > 0:
        free = [i for i in range(1, count) if given[i] < largest] or [i for i in range(1, count) if given[i] < reach]
        pool, left = sum([portions[i] for i in free]), rest
        for i in free:
            addition = min(reach - given[i], max(1, left * portions[i] // pool), rest)
            given[i] = given[i] + addition
            rest = rest - addition
    return np.array(given)


def bell_draw(rng, extent, width, bound, split=(), held_as=jnp.bfloat16):
    values = jax.random.normal(rng, extent, jnp.float32) * width
    if len(split) > 0:
        values = block_scale(rng, extent, split, -0.22, 0.18) * values
    return jnp.clip(values, min=-bound, max=bound).astype(held_as)


def setup_inputs(seed: int = 0) -> dict:
    streams_of = jax.random.split(jax.random.key(seed), 5)
    table = bell_draw(streams_of[0], (TABLES, ROWS, E), 1.0, 6.0, ((0, 8), (1, 16)), jnp.float32)
    row_shard_keys = jax.random.split(jax.random.fold_in(streams_of[1], 1), TABLES * LOOKUPS // LOOK_BLK)
    row_shard_turns = jax.random.permutation(jax.random.fold_in(streams_of[1], 3), TABLES * LOOKUPS // LOOK_BLK)
    row_shard = jax.vmap(lambda own, number: assign_block(jax.random.fold_in(streams_of[1], 2), own, number, LOOK_BLK, N_ROW, 1, CAP, 2))(row_shard_keys, row_shard_turns).reshape((TABLES, LOOKUPS, 1))
    row_offset = place_ends(jax.random.randint(streams_of[2], (TABLES, LOOKUPS), 0, ROWS_DEV), jax.random.fold_in(streams_of[2], 1), 0, ROWS_DEV - 1).astype(jnp.int32)
    bag_lengths = jax.vmap(lambda own: ragged(own, BAGS_BLK, LOOK_BLK, 2 * POOL, 1))(jax.random.split(streams_of[3], TABLES * BLOCKS)).reshape((TABLES, BLOCKS, BAGS_BLK)).astype(jnp.int32)
    return dict(table=table, row_shard=row_shard, row_offset=row_offset, bag_lengths=bag_lengths)


def pool_one(packed):
    matrix, shard_ids, offsets, lengths = packed
    row_index = shard_ids[:, 0] * ROWS_DEV + offsets
    vectors = jnp.take(matrix, row_index, axis=0)
    ends = jnp.cumsum(lengths, axis=-1).astype(jnp.int32)
    places = jnp.arange(LOOK_BLK, dtype=jnp.int32)
    within = jnp.sum((ends[:, None, :] <= places[None, :, None]).astype(jnp.int32), axis=-1).astype(jnp.int32)
    bag_index = within + (jnp.arange(BLOCKS, dtype=jnp.int32) * BAGS_BLK)[:, None]
    return jax.ops.segment_sum(vectors, bag_index.reshape(-1), num_segments=BAGS)


def reference(table, row_shard, row_offset, bag_lengths):
    return lax.map(pool_one, (table, row_shard, row_offset, bag_lengths))
```

```python
import functools

import jax
import jax.numpy as jnp
from jax import lax
from jax.experimental import pallas as pl
from jax.experimental.pallas import tpu as pltpu
from jax.sharding import PartitionSpec as P

AXES = ("grp", "row")
F32 = jnp.float32
BF16 = jnp.bfloat16
NT = (((1,), (1,)), ((), ()))
VMEM_LIMIT = 56 * 1024 * 1024


def list_kernel(cap, me_ref, shard_ref, offset_ref, list_ref, key_s, off_s):
    tables, blocks, look = shard_ref.shape
    me = me_ref[0]
    later = lax.broadcasted_iota(jnp.int32, (look, look), 0)
    earlier = lax.broadcasted_iota(jnp.int32, (look, look), 1)
    tri = (earlier < later).astype(F32).astype(BF16)
    places = [(lax.broadcasted_iota(jnp.int32, (8, blocks), 0) + 8 * i).astype(F32) for i in range(cap // 8)]
    for t in range(tables):
        hit = (shard_ref[t] == me).astype(F32)
        rank = lax.dot_general(tri, hit.astype(BF16), NT, preferred_element_type=F32)
        key_s[...] = jnp.where(jnp.transpose(hit) > 0.5, rank, -1.0)
        off_s[...] = jnp.transpose(offset_ref[t].astype(F32))

        def step(i, accs):
            for u in range(8):
                key = key_s[pl.ds(i * 8 + u, 1), :]
                off = off_s[pl.ds(i * 8 + u, 1), :]
                accs = tuple(jnp.where(key == pos, off, acc) for acc, pos in zip(accs, places))
            return accs

        accs = lax.fori_loop(0, look // 8, step, tuple(jnp.zeros((8, blocks), F32) for _ in places))
        for i, acc in enumerate(accs):
            list_ref[t, pl.ds(8 * i, 8), :] = acc.astype(jnp.int32)


def make_lists(me, shard, offset, cap):
    tables, blocks, look = shard.shape
    return pl.pallas_call(
        functools.partial(list_kernel, cap),
        out_shape=jax.ShapeDtypeStruct((tables, cap, blocks), jnp.int32),
        in_specs=[
            pl.BlockSpec(memory_space=pltpu.SMEM),
            pl.BlockSpec(memory_space=pltpu.VMEM),
            pl.BlockSpec(memory_space=pltpu.VMEM),
        ],
        out_specs=pl.BlockSpec(memory_space=pltpu.VMEM),
        scratch_shapes=[pltpu.VMEM((look, blocks), F32), pltpu.VMEM((look, blocks), F32)],
        cost_estimate=pl.CostEstimate(flops=20_000_000, bytes_accessed=600_000, transcendentals=0),
        name="lists",
    )(me, shard, offset)


def gather_kernel(cap, per_step, list_ref, table_ref, out_ref):
    first = pl.program_id(0) * per_step

    def one(k, carry):
        for j in range(cap):
            row = list_ref[j, first + k]
            out_ref[pl.ds(k * cap + j, 1), :] = table_ref[0, pl.ds(row, 1), :]
        return carry

    lax.fori_loop(0, per_step, one, 0)


def gather_rows(lists, table, t, steps):
    cap, blocks = lists.shape
    _, rows, width = table.shape
    per_step = blocks // steps
    return pl.pallas_call(
        functools.partial(gather_kernel, cap, per_step),
        grid=(steps,),
        out_shape=jax.ShapeDtypeStruct((blocks * cap, width), F32),
        in_specs=[
            pl.BlockSpec(memory_space=pltpu.SMEM),
            pl.BlockSpec((1, rows, width), lambda i: (t, 0, 0)),
        ],
        out_specs=pl.BlockSpec((per_step * cap, width), lambda i: (i, 0)),
        compiler_params=pltpu.CompilerParams(vmem_limit_bytes=VMEM_LIMIT),
        cost_estimate=pl.CostEstimate(flops=40_000_000, bytes_accessed=8_000_000, transcendentals=0),
        name="gather",
    )(lists, table)


def weight_kernel(cap, shards, shard_ref, length_ref, out_ref):
    look = shard_ref.shape[2]
    bags = length_ref.shape[2]
    shard = shard_ref[0].astype(F32)
    ids = lax.broadcasted_iota(jnp.int32, (shards, look), 0).astype(F32)
    hit = (shard == ids).astype(F32)
    row = lax.broadcasted_iota(jnp.int32, (look, look), 0)
    col = lax.broadcasted_iota(jnp.int32, (look, look), 1)
    upper = (row < col).astype(F32).astype(BF16)
    before = jnp.dot(hit.astype(BF16), upper, preferred_element_type=F32)
    slot = jnp.sum(hit * before, axis=0, keepdims=True) + shard * cap
    places = lax.broadcasted_iota(jnp.int32, (shards * cap, look), 0).astype(F32)
    chosen = (places == slot).astype(F32).astype(BF16)
    brow = lax.broadcasted_iota(jnp.int32, (bags, bags), 0)
    bcol = lax.broadcasted_iota(jnp.int32, (bags, bags), 1)
    length = length_ref[0].astype(F32)
    ends = jnp.sum(jnp.where(bcol <= brow, length, 0.0), axis=1, keepdims=True)
    starts = jnp.sum(jnp.where(bcol < brow, length, 0.0), axis=1, keepdims=True)
    spot = lax.broadcasted_iota(jnp.int32, (bags, look), 1).astype(F32)
    inside = ((spot >= starts) & (spot < ends)).astype(F32).astype(BF16)
    out_ref[0] = lax.dot_general(inside, chosen, NT, preferred_element_type=F32).astype(BF16)


def make_weights(shard, length, cap, shards):
    tables, _, look = shard.shape
    bags = length.shape[2]
    return pl.pallas_call(
        functools.partial(weight_kernel, cap, shards),
        grid=(tables,),
        out_shape=jax.ShapeDtypeStruct((tables, bags, shards * cap), BF16),
        in_specs=[
            pl.BlockSpec((1, 1, look), lambda i: (i, 0, 0)),
            pl.BlockSpec((1, 1, bags), lambda i: (i, 0, 0)),
        ],
        out_specs=pl.BlockSpec((1, bags, shards * cap), lambda i: (i, 0, 0)),
        cost_estimate=pl.CostEstimate(flops=30_000_000, bytes_accessed=3_000_000, transcendentals=0),
        name="weights",
    )(shard, length)


def pool_kernel(weight_ref, rows_ref, out_ref):
    rows = rows_ref[0]
    high = rows.astype(BF16)
    low = (rows - high.astype(F32)).astype(BF16)
    weight = weight_ref[0, 0]
    out_ref[0, 0] = jnp.dot(weight, high, preferred_element_type=F32) + jnp.dot(
        weight, low, preferred_element_type=F32
    )


def pool_kernel_into(weight_ref, rows_ref, held_ref, out_ref):
    pool_kernel(weight_ref, rows_ref, out_ref)


def pool(weights, rows, t, held):
    groups, per_group, bags, slots = weights.shape
    width = rows.shape[2]
    in_specs = [
        pl.BlockSpec((1, 1, bags, slots), lambda i: (i, t, 0, 0)),
        pl.BlockSpec((1, slots, width), lambda i: (i, 0, 0)),
    ]
    args = [weights, rows]
    if held is not None:
        in_specs.append(pl.BlockSpec(memory_space=pl.ANY))
        args.append(held)
    return pl.pallas_call(
        pool_kernel if held is None else pool_kernel_into,
        grid=(groups,),
        out_shape=jax.ShapeDtypeStruct((groups, per_group, bags, width), F32),
        in_specs=in_specs,
        out_specs=pl.BlockSpec((1, 1, bags, width), lambda i: (i, t, 0, 0)),
        input_output_aliases={} if held is None else {2: 0},
        cost_estimate=pl.CostEstimate(flops=20_000_000, bytes_accessed=4_000_000, transcendentals=0),
        name="pool",
    )(*args)


def body(table, row_shard, row_offset, bag_lengths):
    groups = lax.axis_size("grp")
    shards = lax.axis_size("row")
    mine = lax.axis_index("row")
    tables, _, width = table.shape
    blocks, bags = bag_lengths.shape[1:]
    look = row_offset.shape[1] // blocks
    cap = 3 * look // shards
    shard = row_shard.reshape(tables, blocks, look)
    offset = row_offset.reshape(tables, blocks, look)

    per_owner = (tables, groups, shards)
    own = jnp.concatenate(
        [
            lax.dynamic_index_in_dim(shard.reshape(*per_owner, look), mine, 2, keepdims=False),
            lax.dynamic_index_in_dim(bag_lengths.reshape(*per_owner, bags), mine, 2, keepdims=False),
        ],
        axis=2,
    )
    about = lax.all_to_all(own.transpose(1, 0, 2), "grp", 0, 0, tiled=True)
    about = about.reshape(groups * tables, 1, look + bags)
    weights = make_weights(about[..., :look], about[..., look:], cap, shards)
    weights = weights.reshape(groups, tables, bags, shards * cap)

    lists = make_lists(mine.reshape(1), shard, offset, cap)
    moved = []
    for t in range(tables):
        rows = gather_rows(lists[t], table, t, 8).reshape(blocks, cap, width)
        moved.append(lax.all_to_all(rows, AXES, 0, 0, tiled=True))
    out = None
    for t in range(tables):
        out = pool(weights, moved[t].reshape(groups, shards * cap, width), t, out)
    return out.reshape(groups * tables, bags, width)


def solution(mesh):
    placed = (P("grp", "row", None), P("grp", None, None), P("grp", None), P("grp", None, None))
    return jax.shard_map(
        body, mesh=mesh, in_specs=placed, out_specs=P(None, AXES, None), check_vma=False
    )
```

```python
import functools

import jax
import jax.numpy as jnp
from jax import lax
from jax.experimental import pallas as pl
from jax.experimental.pallas import tpu as pltpu
from jax.sharding import PartitionSpec as P

AXES = ("grp", "row")
F32 = jnp.float32
BF16 = jnp.bfloat16
NT = (((1,), (1,)), ((), ()))
VMEM_LIMIT = 56 * 1024 * 1024
LANES = 128
PIECES = 8


def front_kernel(tables, blocks, cap, me_ref, shard_ref, offset_ref, table_ref, out_ref,
                 key_s, off_s, list_v, list_s, held, rows, table_sem, list_sem, out_sem):
    look = key_s.shape[0]
    halves = look // LANES
    size = table_ref.shape[1]
    me = me_ref[0]
    fetch = [
        pltpu.make_async_copy(table_ref.at[t], held.at[pl.ds(t * size, size)], table_sem.at[t])
        for t in range(tables)
    ]
    for copy in fetch:
        copy.start()
    later = lax.broadcasted_iota(jnp.int32, (look, look), 0)
    earlier = lax.broadcasted_iota(jnp.int32, (look, look), 1)
    tri = (earlier < later).astype(F32).astype(BF16)
    places = [(lax.broadcasted_iota(jnp.int32, (8, blocks), 0) + 8 * i).astype(F32) for i in range(cap // 8)]
    for t in range(tables):
        hit = jnp.concatenate(
            [(shard_ref[t, pl.ds(h, blocks, stride=halves), :] == me).astype(F32) for h in range(halves)], axis=1
        )
        rank = lax.dot_general(tri, hit.astype(BF16), NT, preferred_element_type=F32)
        key_s[...] = jnp.where(jnp.transpose(hit) > 0.5, rank, -1.0)
        for h in range(halves):
            off = offset_ref[pl.ds(h * tables + t, blocks, stride=halves * tables), :] + t * size
            off_s[pl.ds(h * LANES, LANES), :] = jnp.transpose(off.astype(F32))

        def step(i, accs):
            for u in range(8):
                key = key_s[pl.ds(i * 8 + u, 1), :]
                off = off_s[pl.ds(i * 8 + u, 1), :]
                accs = tuple(jnp.where(key == pos, off, acc) for acc, pos in zip(accs, places))
            return accs

        accs = lax.fori_loop(0, look // 8, step, tuple(jnp.zeros((8, blocks), F32) for _ in places))
        whole = jnp.concatenate(list(accs) + [jnp.zeros((LANES - cap, blocks), F32)], axis=0)
        list_v[pl.ds(t * blocks, blocks), :] = jnp.transpose(whole).astype(jnp.int32)
    listed = pltpu.make_async_copy(list_v, list_s, list_sem)
    listed.start()
    listed.wait()
    for copy in fetch:
        copy.wait()

    per_piece = blocks // PIECES
    per_block = tables * cap

    def block(k, carry):
        for t in range(tables):
            for j in range(cap):
                row = list_s[t * blocks + k, j]
                rows[pl.ds(k * per_block + t * cap + j, 1), :] = held[pl.ds(row, 1), :]
        return carry

    sends = []
    for i in range(PIECES):
        lax.fori_loop(i * per_piece, (i + 1) * per_piece, block, 0)
        part = pl.ds(i * per_piece * per_block, per_piece * per_block)
        copy = pltpu.make_async_copy(rows.at[part], out_ref.at[part], out_sem.at[i])
        copy.start()
        sends.append(copy)
    for copy in sends:
        copy.wait()


def front(me, shard, offset, table, blocks, cap):
    tables, size, width = table.shape
    look = shard.shape[1] * LANES // blocks
    return pl.pallas_call(
        functools.partial(front_kernel, tables, blocks, cap),
        out_shape=jax.ShapeDtypeStruct((blocks * tables * cap, width), F32),
        in_specs=[
            pl.BlockSpec(memory_space=pltpu.SMEM),
            pl.BlockSpec(memory_space=pltpu.VMEM),
            pl.BlockSpec(memory_space=pltpu.VMEM),
            pl.BlockSpec(memory_space=pl.ANY),
        ],
        out_specs=pl.BlockSpec(memory_space=pl.ANY),
        scratch_shapes=[
            pltpu.VMEM((look, blocks), F32),
            pltpu.VMEM((look, blocks), F32),
            pltpu.VMEM((tables * blocks, LANES), jnp.int32),
            pltpu.SMEM((tables * blocks, LANES), jnp.int32),
            pltpu.VMEM((tables * size, width), F32),
            pltpu.VMEM((blocks * tables * cap, width), F32),
            pltpu.SemaphoreType.DMA((tables,)),
            pltpu.SemaphoreType.DMA,
            pltpu.SemaphoreType.DMA((PIECES,)),
        ],
        compiler_params=pltpu.CompilerParams(vmem_limit_bytes=VMEM_LIMIT),
        cost_estimate=pl.CostEstimate(flops=60_000_000, bytes_accessed=15_000_000, transcendentals=0),
        name="front",
    )(me, shard, offset, table)


def weight_kernel(cap, shards, shard_ref, length_ref, out_ref):
    look = shard_ref.shape[2]
    bags = length_ref.shape[2]
    shard = shard_ref[0].astype(F32)
    ids = lax.broadcasted_iota(jnp.int32, (shards, look), 0).astype(F32)
    hit = (shard == ids).astype(F32)
    row = lax.broadcasted_iota(jnp.int32, (look, look), 0)
    col = lax.broadcasted_iota(jnp.int32, (look, look), 1)
    upper = (row < col).astype(F32).astype(BF16)
    before = jnp.dot(hit.astype(BF16), upper, preferred_element_type=F32)
    slot = jnp.sum(hit * before, axis=0, keepdims=True) + shard * cap
    places = lax.broadcasted_iota(jnp.int32, (shards * cap, look), 0).astype(F32)
    chosen = (places == slot).astype(F32).astype(BF16)
    brow = lax.broadcasted_iota(jnp.int32, (bags, bags), 0)
    bcol = lax.broadcasted_iota(jnp.int32, (bags, bags), 1)
    length = length_ref[0].astype(F32)
    ends = jnp.sum(jnp.where(bcol <= brow, length, 0.0), axis=1, keepdims=True)
    starts = jnp.sum(jnp.where(bcol < brow, length, 0.0), axis=1, keepdims=True)
    spot = lax.broadcasted_iota(jnp.int32, (bags, look), 1).astype(F32)
    inside = ((spot >= starts) & (spot < ends)).astype(F32).astype(BF16)
    out_ref[0] = lax.dot_general(inside, chosen, NT, preferred_element_type=F32).astype(BF16)


def make_weights(shard, length, cap, shards):
    tables, _, look = shard.shape
    bags = length.shape[2]
    return pl.pallas_call(
        functools.partial(weight_kernel, cap, shards),
        grid=(tables,),
        out_shape=jax.ShapeDtypeStruct((tables, bags, shards * cap), BF16),
        in_specs=[
            pl.BlockSpec((1, 1, look), lambda i: (i, 0, 0)),
            pl.BlockSpec((1, 1, bags), lambda i: (i, 0, 0)),
        ],
        out_specs=pl.BlockSpec((1, bags, shards * cap), lambda i: (i, 0, 0)),
        cost_estimate=pl.CostEstimate(flops=30_000_000, bytes_accessed=3_000_000, transcendentals=0),
        name="weights",
    )(shard, length)


def pool_kernel(tables, cap, weight_ref, rows_ref, out_ref):
    shards, _, width = rows_ref.shape
    for t in range(tables):
        rows = rows_ref[:, pl.ds(t * cap, cap), :].reshape(shards * cap, width)
        high = rows.astype(BF16)
        low = (rows - high.astype(F32)).astype(BF16)
        both = jnp.dot(weight_ref[t], jnp.concatenate([high, low], axis=1), preferred_element_type=F32)
        out_ref[t] = both[:, :width] + both[:, width:]


def pool(weights, rows, groups, cap):
    total, bags, slots = weights.shape
    tables = total // groups
    shards = rows.shape[0] // groups
    width = rows.shape[2]
    return pl.pallas_call(
        functools.partial(pool_kernel, tables, cap),
        grid=(groups,),
        out_shape=jax.ShapeDtypeStruct((total, bags, width), F32),
        in_specs=[
            pl.BlockSpec((tables, bags, slots), lambda i: (i, 0, 0)),
            pl.BlockSpec((shards, tables * cap, width), lambda i: (i, 0, 0)),
        ],
        out_specs=pl.BlockSpec((tables, bags, width), lambda i: (i, 0, 0)),
        cost_estimate=pl.CostEstimate(flops=20_000_000, bytes_accessed=4_000_000, transcendentals=0),
        name="pool",
    )(weights, rows)


def body(table, row_shard, row_offset, bag_lengths):
    groups = lax.axis_size("grp")
    shards = lax.axis_size("row")
    mine = lax.axis_index("row")
    tables, _, width = table.shape
    blocks, bags = bag_lengths.shape[1:]
    lookups = row_offset.shape[1]
    look = lookups // blocks
    cap = 3 * look // shards

    shard = row_shard.reshape(tables, lookups // LANES, LANES)
    offset = row_offset.reshape(tables, lookups // LANES, LANES).transpose(1, 0, 2)
    rows = front(mine.reshape(1), shard, offset.reshape(-1, LANES), table, blocks, cap)
    moved = lax.all_to_all(rows.reshape(blocks, tables * cap, width), AXES, 0, 0, tiled=True)

    per_owner = (tables, groups, shards)
    own = jnp.concatenate(
        [
            lax.dynamic_index_in_dim(row_shard.reshape(*per_owner, look), mine, 2, keepdims=False),
            lax.dynamic_index_in_dim(bag_lengths.reshape(*per_owner, bags), mine, 2, keepdims=False),
        ],
        axis=2,
    )
    about = lax.all_to_all(own.transpose(1, 0, 2), "grp", 0, 0, tiled=True)
    about = about.reshape(groups * tables, 1, look + bags)
    weights = make_weights(about[..., :look], about[..., look:], cap, shards)
    return pool(weights, moved, groups, cap)


def solution(mesh):
    placed = (P("grp", "row", None), P("grp", None, None), P("grp", None), P("grp", None, None))
    return jax.shard_map(
        body, mesh=mesh, in_specs=placed, out_specs=P(None, AXES, None), check_vma=False
    )
```

```python
import functools

import jax
import jax.numpy as jnp
from jax import lax
from jax.experimental import pallas as pl
from jax.experimental.pallas import tpu as pltpu
from jax.sharding import PartitionSpec as P

AXES = ("grp", "row")
F32 = jnp.float32
BF16 = jnp.bfloat16
NT = (((1,), (1,)), ((), ()))
VMEM_LIMIT = 56 * 1024 * 1024
LANES = 128
PIECES = 8


def front_kernel(tables, blocks, cap, me_ref, shard_ref, offset_ref, table_ref, out_ref,
                 key_s, off_s, list_v, list_s, held, rows, table_sem, list_sem, out_sem):
    look = key_s.shape[0]
    halves = look // LANES
    size = table_ref.shape[1]
    me = me_ref[0]
    fetch = [
        pltpu.make_async_copy(table_ref.at[t], held.at[pl.ds(t * size, size)], table_sem.at[t])
        for t in range(tables)
    ]
    for copy in fetch:
        copy.start()
    later = lax.broadcasted_iota(jnp.int32, (look, look), 0)
    earlier = lax.broadcasted_iota(jnp.int32, (look, look), 1)
    tri = (earlier < later).astype(F32).astype(BF16)
    places = [(lax.broadcasted_iota(jnp.int32, (8, blocks), 0) + 8 * i).astype(F32) for i in range(cap // 8)]
    for t in range(tables):
        hit = jnp.concatenate(
            [(shard_ref[t, pl.ds(h, blocks, stride=halves), :] == me).astype(F32) for h in range(halves)], axis=1
        )
        rank = lax.dot_general(tri, hit.astype(BF16), NT, preferred_element_type=F32)
        key_s[...] = jnp.where(jnp.transpose(hit) > 0.5, rank, -1.0)
        for h in range(halves):
            off = offset_ref[pl.ds(h * tables + t, blocks, stride=halves * tables), :] + t * size
            off_s[pl.ds(h * LANES, LANES), :] = jnp.transpose(off.astype(F32))

        def step(i, accs):
            for u in range(8):
                key = key_s[pl.ds(i * 8 + u, 1), :]
                off = off_s[pl.ds(i * 8 + u, 1), :]
                accs = tuple(jnp.where(key == pos, off, acc) for acc, pos in zip(accs, places))
            return accs

        accs = lax.fori_loop(0, look // 8, step, tuple(jnp.zeros((8, blocks), F32) for _ in places))
        whole = jnp.concatenate(list(accs) + [jnp.zeros((LANES - cap, blocks), F32)], axis=0)
        list_v[pl.ds(t * blocks, blocks), :] = jnp.transpose(whole).astype(jnp.int32)
    listed = pltpu.make_async_copy(list_v, list_s, list_sem)
    listed.start()
    listed.wait()
    for copy in fetch:
        copy.wait()

    per_piece = blocks // PIECES
    per_block = tables * cap

    def block(k, carry):
        for t in range(tables):
            for j in range(cap):
                row = list_s[t * blocks + k, j]
                rows[pl.ds(k * per_block + t * cap + j, 1), :] = held[pl.ds(row, 1), :]
        return carry

    sends = []
    for i in range(PIECES):
        lax.fori_loop(i * per_piece, (i + 1) * per_piece, block, 0)
        part = pl.ds(i * per_piece * per_block, per_piece * per_block)
        copy = pltpu.make_async_copy(rows.at[part], out_ref.at[part], out_sem.at[i])
        copy.start()
        sends.append(copy)
    for copy in sends:
        copy.wait()


def front(me, shard, offset, table, blocks, cap):
    tables, size, width = table.shape
    look = shard.shape[1] * LANES // blocks
    return pl.pallas_call(
        functools.partial(front_kernel, tables, blocks, cap),
        out_shape=jax.ShapeDtypeStruct((blocks * tables * cap, width), F32),
        in_specs=[
            pl.BlockSpec(memory_space=pltpu.SMEM),
            pl.BlockSpec(memory_space=pltpu.VMEM),
            pl.BlockSpec(memory_space=pltpu.VMEM),
            pl.BlockSpec(memory_space=pl.ANY),
        ],
        out_specs=pl.BlockSpec(memory_space=pl.ANY),
        scratch_shapes=[
            pltpu.VMEM((look, blocks), F32),
            pltpu.VMEM((look, blocks), F32),
            pltpu.VMEM((tables * blocks, LANES), jnp.int32),
            pltpu.SMEM((tables * blocks, LANES), jnp.int32),
            pltpu.VMEM((tables * size, width), F32),
            pltpu.VMEM((blocks * tables * cap, width), F32),
            pltpu.SemaphoreType.DMA((tables,)),
            pltpu.SemaphoreType.DMA,
            pltpu.SemaphoreType.DMA((PIECES,)),
        ],
        compiler_params=pltpu.CompilerParams(vmem_limit_bytes=VMEM_LIMIT),
        cost_estimate=pl.CostEstimate(flops=60_000_000, bytes_accessed=15_000_000, transcendentals=0),
        name="front",
    )(me, shard, offset, table)


def weight_kernel(cap, shards, shard_ref, length_ref, out_ref):
    look = shard_ref.shape[2]
    bags = length_ref.shape[2]
    shard = shard_ref[0].astype(F32)
    ids = lax.broadcasted_iota(jnp.int32, (shards, look), 0).astype(F32)
    hit = (shard == ids).astype(F32)
    row = lax.broadcasted_iota(jnp.int32, (look, look), 0)
    col = lax.broadcasted_iota(jnp.int32, (look, look), 1)
    upper = (row < col).astype(F32).astype(BF16)
    before = jnp.dot(hit.astype(BF16), upper, preferred_element_type=F32)
    slot = jnp.sum(hit * before, axis=0, keepdims=True) + shard * cap
    places = lax.broadcasted_iota(jnp.int32, (shards * cap, look), 0).astype(F32)
    chosen = (places == slot).astype(F32).astype(BF16)
    brow = lax.broadcasted_iota(jnp.int32, (bags, bags), 0)
    bcol = lax.broadcasted_iota(jnp.int32, (bags, bags), 1)
    length = length_ref[0].astype(F32)
    ends = jnp.sum(jnp.where(bcol <= brow, length, 0.0), axis=1, keepdims=True)
    starts = jnp.sum(jnp.where(bcol < brow, length, 0.0), axis=1, keepdims=True)
    spot = lax.broadcasted_iota(jnp.int32, (bags, look), 1).astype(F32)
    inside = ((spot >= starts) & (spot < ends)).astype(F32).astype(BF16)
    out_ref[0] = lax.dot_general(inside, chosen, NT, preferred_element_type=F32).astype(BF16)


def make_weights(shard, length, cap, shards):
    tables, _, look = shard.shape
    bags = length.shape[2]
    return pl.pallas_call(
        functools.partial(weight_kernel, cap, shards),
        grid=(tables,),
        out_shape=jax.ShapeDtypeStruct((tables, bags, shards * cap), BF16),
        in_specs=[
            pl.BlockSpec((1, 1, look), lambda i: (i, 0, 0)),
            pl.BlockSpec((1, 1, bags), lambda i: (i, 0, 0)),
        ],
        out_specs=pl.BlockSpec((1, bags, shards * cap), lambda i: (i, 0, 0)),
        cost_estimate=pl.CostEstimate(flops=30_000_000, bytes_accessed=3_000_000, transcendentals=0),
        name="weights",
    )(shard, length)


def pool_kernel(tables, cap, weight_ref, rows_ref, out_ref):
    shards, _, width = rows_ref.shape
    for t in range(tables):
        rows = rows_ref[:, pl.ds(t * cap, cap), :].reshape(shards * cap, width)
        high = rows.astype(BF16)
        low = (rows - high.astype(F32)).astype(BF16)
        both = jnp.dot(weight_ref[t], jnp.concatenate([high, low], axis=1), preferred_element_type=F32)
        out_ref[t] = both[:, :width] + both[:, width:]


def pool(weights, rows, groups, cap):
    total, bags, slots = weights.shape
    tables = total // groups
    shards = rows.shape[0] // groups
    width = rows.shape[2]
    return pl.pallas_call(
        functools.partial(pool_kernel, tables, cap),
        grid=(groups,),
        out_shape=jax.ShapeDtypeStruct((total, bags, width), F32),
        in_specs=[
            pl.BlockSpec((tables, bags, slots), lambda i: (i, 0, 0)),
            pl.BlockSpec((shards, tables * cap, width), lambda i: (i, 0, 0)),
        ],
        out_specs=pl.BlockSpec((tables, bags, width), lambda i: (i, 0, 0)),
        cost_estimate=pl.CostEstimate(flops=20_000_000, bytes_accessed=4_000_000, transcendentals=0),
        name="pool",
    )(weights, rows)


def body(table, row_shard, row_offset, bag_lengths):
    groups = lax.axis_size("grp")
    shards = lax.axis_size("row")
    mine = lax.axis_index("row")
    tables, _, width = table.shape
    blocks, bags = bag_lengths.shape[1:]
    lookups = row_offset.shape[1]
    look = lookups // blocks
    cap = 3 * look // shards

    shard = row_shard.reshape(tables, lookups // LANES, LANES)
    offset = row_offset.reshape(tables, lookups // LANES, LANES).transpose(1, 0, 2)
    rows = front(mine.reshape(1), shard, offset.reshape(-1, LANES), table, blocks, cap)
    rows, shard, bag_lengths = lax.optimization_barrier((rows, shard, bag_lengths))
    moved = lax.all_to_all(rows.reshape(blocks, tables * cap, width), AXES, 0, 0, tiled=True)

    halves = look // LANES
    own = jnp.concatenate(
        [
            lax.dynamic_slice_in_dim(
                shard.reshape(tables, groups, shards * halves, LANES), mine * halves, halves, 2
            ).reshape(tables, groups, look),
            lax.dynamic_index_in_dim(
                bag_lengths.reshape(tables, groups, shards, bags), mine, 2, keepdims=False
            ),
        ],
        axis=2,
    )
    every = lax.all_gather(own, "grp")
    about = lax.dynamic_index_in_dim(every, lax.axis_index("grp"), 2, keepdims=False)
    about = about.reshape(groups * tables, 1, look + bags)
    weights = make_weights(about[..., :look], about[..., look:], cap, shards)
    return pool(weights, moved, groups, cap)


def solution(mesh):
    placed = (P("grp", "row", None), P("grp", None, None), P("grp", None), P("grp", None, None))
    return jax.shard_map(
        body, mesh=mesh, in_specs=placed, out_specs=P(None, AXES, None), check_vma=False
    )
```

```python
import functools

import jax
import jax.numpy as jnp
from jax import lax
from jax.experimental import pallas as pl
from jax.experimental.pallas import tpu as pltpu
from jax.sharding import PartitionSpec as P

AXES = ("grp", "row")
F32 = jnp.float32
BF16 = jnp.bfloat16
NT = (((1,), (1,)), ((), ()))
VMEM_LIMIT = 56 * 1024 * 1024
LANES = 128
FETCHES = 8


def front_kernel(tables, blocks, cap, me_ref, shard_ref, offset_ref, table_ref, out_ref,
                 key_s, off_s, list_v, held, rows, index_0, index_1, index_2, index_3,
                 table_sem, list_sem, out_sem):
    indices = (index_0, index_1, index_2, index_3)
    look = key_s.shape[0]
    halves = look // LANES
    size = table_ref.shape[1]
    me = me_ref[0]
    part = tables * size // FETCHES
    fetch = []
    for i in range(FETCHES):
        t, at = divmod(i * part, size)
        fetch.append(
            pltpu.make_async_copy(
                table_ref.at[t, pl.ds(at, part)], held.at[pl.ds(i * part, part)], table_sem.at[i]
            )
        )
    for copy in fetch:
        copy.start()
    later = lax.broadcasted_iota(jnp.int32, (look, look), 0)
    earlier = lax.broadcasted_iota(jnp.int32, (look, look), 1)
    tri = (earlier < later).astype(F32).astype(BF16)
    places = [(lax.broadcasted_iota(jnp.int32, (8, blocks), 0) + 8 * i).astype(F32) for i in range(cap // 8)]
    listed = []
    for t in range(tables):
        hit = jnp.concatenate(
            [(shard_ref[t, pl.ds(h, blocks, stride=halves), :] == me).astype(F32) for h in range(halves)], axis=1
        )
        rank = lax.dot_general(tri, hit.astype(BF16), NT, preferred_element_type=F32)
        key_s[...] = jnp.where(jnp.transpose(hit) > 0.5, rank, -1.0)
        for h in range(halves):
            off = offset_ref[pl.ds(h * tables + t, blocks, stride=halves * tables), :] + t * size
            off_s[pl.ds(h * LANES, LANES), :] = jnp.transpose(off.astype(F32))

        def step(i, accs):
            for u in range(8):
                key = key_s[pl.ds(i * 8 + u, 1), :]
                off = off_s[pl.ds(i * 8 + u, 1), :]
                accs = tuple(jnp.where(key == pos, off, acc) for acc, pos in zip(accs, places))
            return accs

        listed += lax.fori_loop(0, look // 8, step, tuple(jnp.zeros((8, blocks), F32) for _ in places))
    listed.append(jnp.zeros((LANES - tables * cap, blocks), F32))
    list_v[...] = jnp.transpose(jnp.concatenate(listed, axis=0)).astype(jnp.int32)

    per_block = tables * cap
    per_tile = 8 * per_block
    tiles = blocks // 8

    def index_copy(tile, slot):
        return pltpu.make_async_copy(list_v.at[pl.ds(tile * 8, 8)], indices[slot], list_sem.at[slot])

    def out_copy(tile):
        span = pl.ds(tile * per_tile, per_tile)
        return pltpu.make_async_copy(rows.at[span], out_ref.at[span], out_sem.at[tile])

    for slot in range(4):
        index_copy(slot, slot).start()
    for copy in fetch:
        copy.wait()

    def four(i, carry):
        for slot in range(4):
            tile = i * 4 + slot
            index_copy(tile, slot).wait()
            for u in range(8):
                for j in range(per_block):
                    row = indices[slot][u, j]
                    rows[pl.ds(tile * per_tile + u * per_block + j, 1), :] = held[pl.ds(row, 1), :]
            out_copy(tile).start()

            @pl.when(tile + 4 < tiles)
            def _():
                index_copy(tile + 4, slot).start()

        return carry

    lax.fori_loop(0, tiles // 4, four, 0)
    for tile in range(tiles):
        out_copy(tile).wait()


def front(me, shard, offset, table, blocks, cap):
    tables, size, width = table.shape
    look = shard.shape[1] * LANES // blocks
    return pl.pallas_call(
        functools.partial(front_kernel, tables, blocks, cap),
        out_shape=jax.ShapeDtypeStruct((blocks * tables * cap, width), F32),
        in_specs=[
            pl.BlockSpec(memory_space=pltpu.SMEM),
            pl.BlockSpec(memory_space=pltpu.VMEM),
            pl.BlockSpec(memory_space=pltpu.VMEM),
            pl.BlockSpec(memory_space=pl.ANY),
        ],
        out_specs=pl.BlockSpec(memory_space=pl.ANY),
        scratch_shapes=[
            pltpu.VMEM((look, blocks), F32),
            pltpu.VMEM((look, blocks), F32),
            pltpu.VMEM((blocks, LANES), jnp.int32),
            pltpu.VMEM((tables * size, width), F32),
            pltpu.VMEM((blocks * tables * cap, width), F32),
        ]
        + [pltpu.SMEM((8, LANES), jnp.int32)] * 4
        + [
            pltpu.SemaphoreType.DMA((FETCHES,)),
            pltpu.SemaphoreType.DMA((4,)),
            pltpu.SemaphoreType.DMA((blocks // 8,)),
        ],
        compiler_params=pltpu.CompilerParams(vmem_limit_bytes=VMEM_LIMIT),
        cost_estimate=pl.CostEstimate(flops=60_000_000, bytes_accessed=15_000_000, transcendentals=0),
        name="front",
    )(me, shard, offset, table)


def weight_kernel(cap, shards, shard_ref, length_ref, out_ref):
    look = shard_ref.shape[2]
    bags = length_ref.shape[2]
    shard = shard_ref[0].astype(F32)
    ids = lax.broadcasted_iota(jnp.int32, (shards, look), 0).astype(F32)
    hit = (shard == ids).astype(F32)
    row = lax.broadcasted_iota(jnp.int32, (look, look), 0)
    col = lax.broadcasted_iota(jnp.int32, (look, look), 1)
    upper = (row < col).astype(F32).astype(BF16)
    before = jnp.dot(hit.astype(BF16), upper, preferred_element_type=F32)
    slot = jnp.sum(hit * before, axis=0, keepdims=True) + shard * cap
    places = lax.broadcasted_iota(jnp.int32, (shards * cap, look), 0).astype(F32)
    chosen = (places == slot).astype(F32).astype(BF16)
    brow = lax.broadcasted_iota(jnp.int32, (bags, bags), 0)
    bcol = lax.broadcasted_iota(jnp.int32, (bags, bags), 1)
    length = length_ref[0].astype(F32)
    ends = jnp.sum(jnp.where(bcol <= brow, length, 0.0), axis=1, keepdims=True)
    starts = jnp.sum(jnp.where(bcol < brow, length, 0.0), axis=1, keepdims=True)
    spot = lax.broadcasted_iota(jnp.int32, (bags, look), 1).astype(F32)
    inside = ((spot >= starts) & (spot < ends)).astype(F32).astype(BF16)
    out_ref[0] = lax.dot_general(inside, chosen, NT, preferred_element_type=F32).astype(BF16)


def make_weights(shard, length, cap, shards):
    tables, _, look = shard.shape
    bags = length.shape[2]
    return pl.pallas_call(
        functools.partial(weight_kernel, cap, shards),
        grid=(tables,),
        out_shape=jax.ShapeDtypeStruct((tables, bags, shards * cap), BF16),
        in_specs=[
            pl.BlockSpec((1, 1, look), lambda i: (i, 0, 0)),
            pl.BlockSpec((1, 1, bags), lambda i: (i, 0, 0)),
        ],
        out_specs=pl.BlockSpec((1, bags, shards * cap), lambda i: (i, 0, 0)),
        compiler_params=pltpu.CompilerParams(vmem_limit_bytes=16 * 1024 * 1024),
        cost_estimate=pl.CostEstimate(flops=30_000_000, bytes_accessed=3_000_000, transcendentals=0),
        name="weights",
    )(shard, length)


def pool_kernel(groups, tables, cap, weight_ref, rows_ref, out_ref, rows_v, out_v, rows_sem, out_sem):
    width = rows_v.shape[2]
    shards = rows_v.shape[0] // groups

    def rows_copy(g):
        span = pl.ds(g * shards, shards)
        return pltpu.make_async_copy(rows_ref.at[span], rows_v.at[span], rows_sem.at[g])

    def out_copy(g):
        span = pl.ds(g * tables, tables)
        return pltpu.make_async_copy(out_v.at[span], out_ref.at[span], out_sem.at[g])

    for g in range(groups):
        rows_copy(g).start()

    def group(g, carry):
        rows_copy(g).wait()
        for t in range(tables):
            rows = rows_v[pl.ds(g * shards, shards), pl.ds(t * cap, cap), :].reshape(shards * cap, width)
            high = rows.astype(BF16)
            low = (rows - high.astype(F32)).astype(BF16)
            both = jnp.dot(
                weight_ref[g * tables + t], jnp.concatenate([high, low], axis=1), preferred_element_type=F32
            )
            out_v[g * tables + t] = both[:, :width] + both[:, width:]
        out_copy(g).start()
        return carry

    lax.fori_loop(0, groups, group, 0)
    for g in range(groups):
        out_copy(g).wait()


def pool(weights, rows, groups, cap):
    total, bags, _ = weights.shape
    width = rows.shape[2]
    return pl.pallas_call(
        functools.partial(pool_kernel, groups, total // groups, cap),
        out_shape=jax.ShapeDtypeStruct((total, bags, width), F32),
        in_specs=[pl.BlockSpec(memory_space=pltpu.VMEM), pl.BlockSpec(memory_space=pl.ANY)],
        out_specs=pl.BlockSpec(memory_space=pl.ANY),
        scratch_shapes=[
            pltpu.VMEM(rows.shape, F32),
            pltpu.VMEM((total, bags, width), F32),
            pltpu.SemaphoreType.DMA((groups,)),
            pltpu.SemaphoreType.DMA((groups,)),
        ],
        compiler_params=pltpu.CompilerParams(vmem_limit_bytes=40 * 1024 * 1024),
        cost_estimate=pl.CostEstimate(flops=20_000_000, bytes_accessed=4_000_000, transcendentals=0),
        name="pool",
    )(weights, rows)


def body(table, row_shard, row_offset, bag_lengths):
    groups = lax.axis_size("grp")
    shards = lax.axis_size("row")
    mine = lax.axis_index("row")
    tables, _, width = table.shape
    blocks, bags = bag_lengths.shape[1:]
    lookups = row_offset.shape[1]
    look = lookups // blocks
    cap = 3 * look // shards

    shard = row_shard.reshape(tables, lookups // LANES, LANES)
    offset = row_offset.reshape(tables, lookups // LANES, LANES).transpose(1, 0, 2)
    rows = front(mine.reshape(1), shard, offset.reshape(-1, LANES), table, blocks, cap)
    moved = lax.all_to_all(rows.reshape(blocks, tables * cap, width), AXES, 0, 0, tiled=True)

    halves = look // LANES
    own = jnp.concatenate(
        [
            lax.dynamic_slice_in_dim(
                shard.reshape(tables, groups, shards * halves, LANES), mine * halves, halves, 2
            ).reshape(tables, groups, look),
            lax.dynamic_index_in_dim(
                bag_lengths.reshape(tables, groups, shards, bags), mine, 2, keepdims=False
            ),
        ],
        axis=2,
    )
    about = lax.all_to_all(own.transpose(1, 0, 2), "grp", 0, 0, tiled=True)
    about = about.reshape(groups * tables, 1, look + bags)
    weights = make_weights(about[..., :look], about[..., look:], cap, shards)
    return pool(weights, moved, groups, cap)


def solution(mesh):
    placed = (P("grp", "row", None), P("grp", None, None), P("grp", None), P("grp", None, None))
    return jax.shard_map(
        body, mesh=mesh, in_specs=placed, out_specs=P(None, AXES, None), check_vma=False
    )
```

```python
import functools

import jax
import jax.numpy as jnp
from jax import lax
from jax.experimental import pallas as pl
from jax.experimental.pallas import tpu as pltpu
from jax.sharding import PartitionSpec as P

AXES = ("grp", "row")
MOVE = ("row", "grp")
F32 = jnp.float32
BF16 = jnp.bfloat16
NT = (((1,), (1,)), ((), ()))
VMEM_LIMIT = 56 * 1024 * 1024
LANES = 128
FETCHES = 8


def front_kernel(tables, blocks, groups, cap, me_ref, shard_ref, offset_ref, table_ref, out_ref,
                 key_s, off_s, by_block, list_v, held, rows, index_0, index_1, index_2, index_3,
                 table_sem, list_sem, out_sem):
    indices = (index_0, index_1, index_2, index_3)
    look = key_s.shape[0]
    halves = look // LANES
    size = table_ref.shape[1]
    me = me_ref[0]
    part = tables * size // FETCHES
    fetch = []
    for i in range(FETCHES):
        t, at = divmod(i * part, size)
        fetch.append(
            pltpu.make_async_copy(
                table_ref.at[t, pl.ds(at, part)], held.at[pl.ds(i * part, part)], table_sem.at[i]
            )
        )
    for copy in fetch:
        copy.start()
    later = lax.broadcasted_iota(jnp.int32, (look, look), 0)
    earlier = lax.broadcasted_iota(jnp.int32, (look, look), 1)
    tri = (earlier < later).astype(F32).astype(BF16)
    places = [(lax.broadcasted_iota(jnp.int32, (8, blocks), 0) + 8 * i).astype(F32) for i in range(cap // 8)]
    listed = []
    for t in range(tables):
        hit = jnp.concatenate(
            [(shard_ref[t, pl.ds(h, blocks, stride=halves), :] == me).astype(F32) for h in range(halves)], axis=1
        )
        rank = lax.dot_general(tri, hit.astype(BF16), NT, preferred_element_type=F32)
        key_s[...] = jnp.where(jnp.transpose(hit) > 0.5, rank, -1.0)
        for h in range(halves):
            off = offset_ref[pl.ds(h * tables + t, blocks, stride=halves * tables), :] + t * size
            off_s[pl.ds(h * LANES, LANES), :] = jnp.transpose(off.astype(F32))

        def step(i, accs):
            for u in range(8):
                key = key_s[pl.ds(i * 8 + u, 1), :]
                off = off_s[pl.ds(i * 8 + u, 1), :]
                accs = tuple(jnp.where(key == pos, off, acc) for acc, pos in zip(accs, places))
            return accs

        listed += lax.fori_loop(0, look // 8, step, tuple(jnp.zeros((8, blocks), F32) for _ in places))
    listed.append(jnp.zeros((LANES - tables * cap, blocks), F32))
    by_block[...] = jnp.transpose(jnp.concatenate(listed, axis=0)).astype(jnp.int32)
    tiles = blocks // groups
    for tile in range(tiles):
        list_v[pl.ds(tile * groups, groups), :] = by_block[pl.ds(tile, groups, stride=tiles), :]

    per_block = tables * cap
    per_tile = groups * per_block

    def index_copy(tile, slot):
        return pltpu.make_async_copy(list_v.at[pl.ds(tile * groups, groups)], indices[slot], list_sem.at[slot])

    def out_copy(tile):
        span = pl.ds(tile * per_tile, per_tile)
        return pltpu.make_async_copy(rows.at[span], out_ref.at[span], out_sem.at[tile])

    for slot in range(4):
        index_copy(slot, slot).start()
    for t in range(tables):
        for i in range(t * FETCHES // tables, (t + 1) * FETCHES // tables):
            fetch[i].wait()
        last = t == tables - 1

        def four(i, carry):
            for slot in range(4):
                tile = i * 4 + slot
                index_copy(tile, slot).wait()
                for u in range(groups):
                    for j in range(t * cap, (t + 1) * cap):
                        row = indices[slot][u, j]
                        rows[pl.ds(tile * per_tile + u * per_block + j, 1), :] = held[pl.ds(row, 1), :]
                if last:
                    out_copy(tile).start()

                    @pl.when(tile + 4 < tiles)
                    def _():
                        index_copy(tile + 4, slot).start()
                else:
                    index_copy(lax.rem(tile + 4, tiles), slot).start()

            return carry

        lax.fori_loop(0, tiles // 4, four, 0)
    for tile in range(tiles):
        out_copy(tile).wait()


def front(me, shard, offset, table, blocks, groups, cap):
    tables, size, width = table.shape
    look = shard.shape[1] * LANES // blocks
    return pl.pallas_call(
        functools.partial(front_kernel, tables, blocks, groups, cap),
        out_shape=jax.ShapeDtypeStruct((blocks * tables * cap, width), F32),
        in_specs=[
            pl.BlockSpec(memory_space=pltpu.SMEM),
            pl.BlockSpec(memory_space=pltpu.VMEM),
            pl.BlockSpec(memory_space=pltpu.VMEM),
            pl.BlockSpec(memory_space=pl.ANY),
        ],
        out_specs=pl.BlockSpec(memory_space=pl.ANY),
        scratch_shapes=[
            pltpu.VMEM((look, blocks), F32),
            pltpu.VMEM((look, blocks), F32),
            pltpu.VMEM((blocks, LANES), jnp.int32),
            pltpu.VMEM((blocks, LANES), jnp.int32),
            pltpu.VMEM((tables * size, width), F32),
            pltpu.VMEM((blocks * tables * cap, width), F32),
        ]
        + [pltpu.SMEM((groups, LANES), jnp.int32)] * 4
        + [
            pltpu.SemaphoreType.DMA((FETCHES,)),
            pltpu.SemaphoreType.DMA((4,)),
            pltpu.SemaphoreType.DMA((blocks // groups,)),
        ],
        compiler_params=pltpu.CompilerParams(vmem_limit_bytes=VMEM_LIMIT),
        cost_estimate=pl.CostEstimate(flops=60_000_000, bytes_accessed=15_000_000, transcendentals=0),
        name="front",
    )(me, shard, offset, table)


def weight_kernel(cap, shards, shard_ref, length_ref, out_ref):
    look = shard_ref.shape[2]
    bags = length_ref.shape[2]
    shard = shard_ref[0].astype(F32)
    ids = lax.broadcasted_iota(jnp.int32, (shards, look), 0).astype(F32)
    hit = (shard == ids).astype(F32)
    row = lax.broadcasted_iota(jnp.int32, (look, look), 0)
    col = lax.broadcasted_iota(jnp.int32, (look, look), 1)
    upper = (row < col).astype(F32).astype(BF16)
    before = jnp.dot(hit.astype(BF16), upper, preferred_element_type=F32)
    slot = jnp.sum(hit * before, axis=0, keepdims=True) + shard * cap
    places = lax.broadcasted_iota(jnp.int32, (shards * cap, look), 0).astype(F32)
    chosen = (places == slot).astype(F32).astype(BF16)
    brow = lax.broadcasted_iota(jnp.int32, (bags, bags), 0)
    bcol = lax.broadcasted_iota(jnp.int32, (bags, bags), 1)
    length = length_ref[0].astype(F32)
    ends = jnp.sum(jnp.where(bcol <= brow, length, 0.0), axis=1, keepdims=True)
    starts = jnp.sum(jnp.where(bcol < brow, length, 0.0), axis=1, keepdims=True)
    spot = lax.broadcasted_iota(jnp.int32, (bags, look), 1).astype(F32)
    inside = ((spot >= starts) & (spot < ends)).astype(F32).astype(BF16)
    out_ref[0] = lax.dot_general(inside, chosen, NT, preferred_element_type=F32).astype(BF16)


def make_weights(shard, length, cap, shards):
    tables, _, look = shard.shape
    bags = length.shape[2]
    return pl.pallas_call(
        functools.partial(weight_kernel, cap, shards),
        grid=(tables,),
        out_shape=jax.ShapeDtypeStruct((tables, bags, shards * cap), BF16),
        in_specs=[
            pl.BlockSpec((1, 1, look), lambda i: (i, 0, 0)),
            pl.BlockSpec((1, 1, bags), lambda i: (i, 0, 0)),
        ],
        out_specs=pl.BlockSpec((1, bags, shards * cap), lambda i: (i, 0, 0)),
        compiler_params=pltpu.CompilerParams(vmem_limit_bytes=16 * 1024 * 1024),
        cost_estimate=pl.CostEstimate(flops=30_000_000, bytes_accessed=3_000_000, transcendentals=0),
        name="weights",
    )(shard, length)


def pool_kernel(groups, tables, cap, weight_ref, rows_ref, out_ref, rows_v, out_v, rows_sem, out_sem):
    _, shards, _, width = rows_v.shape

    def rows_copy(g):
        return pltpu.make_async_copy(rows_ref.at[:, g], rows_v.at[g], rows_sem.at[g])

    def out_copy(g):
        span = pl.ds(g * tables, tables)
        return pltpu.make_async_copy(out_v.at[span], out_ref.at[span], out_sem.at[g])

    for g in range(groups):
        rows_copy(g).start()

    def group(g, carry):
        rows_copy(g).wait()
        for t in range(tables):
            rows = rows_v[g, :, pl.ds(t * cap, cap), :].reshape(shards * cap, width)
            high = rows.astype(BF16)
            low = (rows - high.astype(F32)).astype(BF16)
            both = jnp.dot(
                weight_ref[g * tables + t], jnp.concatenate([high, low], axis=1), preferred_element_type=F32
            )
            out_v[g * tables + t] = both[:, :width] + both[:, width:]
        out_copy(g).start()
        return carry

    lax.fori_loop(0, groups, group, 0)
    for g in range(groups):
        out_copy(g).wait()


def pool(weights, rows, groups, cap):
    total, bags, _ = weights.shape
    shards, _, slots, width = rows.shape
    return pl.pallas_call(
        functools.partial(pool_kernel, groups, total // groups, cap),
        out_shape=jax.ShapeDtypeStruct((total, bags, width), F32),
        in_specs=[pl.BlockSpec(memory_space=pltpu.VMEM), pl.BlockSpec(memory_space=pl.ANY)],
        out_specs=pl.BlockSpec(memory_space=pl.ANY),
        scratch_shapes=[
            pltpu.VMEM((groups, shards, slots, width), F32),
            pltpu.VMEM((total, bags, width), F32),
            pltpu.SemaphoreType.DMA((groups,)),
            pltpu.SemaphoreType.DMA((groups,)),
        ],
        compiler_params=pltpu.CompilerParams(vmem_limit_bytes=40 * 1024 * 1024),
        cost_estimate=pl.CostEstimate(flops=20_000_000, bytes_accessed=4_000_000, transcendentals=0),
        name="pool",
    )(weights, rows)


def body(table, row_shard, row_offset, bag_lengths):
    groups = lax.axis_size("grp")
    shards = lax.axis_size("row")
    mine = lax.axis_index("row")
    tables, _, width = table.shape
    blocks, bags = bag_lengths.shape[1:]
    lookups = row_offset.shape[1]
    look = lookups // blocks
    cap = 3 * look // shards

    shard = row_shard.reshape(tables, lookups // LANES, LANES)
    offset = row_offset.reshape(tables, lookups // LANES, LANES).transpose(1, 0, 2)
    rows = front(mine.reshape(1), shard, offset.reshape(-1, LANES), table, blocks, groups, cap)
    moved = lax.all_to_all(rows.reshape(blocks, tables * cap, width), MOVE, 0, 0, tiled=True)
    moved = moved.reshape(shards, groups, tables * cap, width)

    halves = look // LANES
    own = jnp.concatenate(
        [
            lax.dynamic_slice_in_dim(
                shard.reshape(tables, groups, shards * halves, LANES), mine * halves, halves, 2
            ).reshape(tables, groups, look),
            lax.dynamic_index_in_dim(
                bag_lengths.reshape(tables, groups, shards, bags), mine, 2, keepdims=False
            ),
        ],
        axis=2,
    )
    about = lax.all_to_all(own.transpose(1, 0, 2), "grp", 0, 0, tiled=True)
    about = about.reshape(groups * tables, 1, look + bags)
    weights = make_weights(about[..., :look], about[..., look:], cap, shards)
    return pool(weights, moved, groups, cap)


def solution(mesh):
    placed = (P("grp", "row", None), P("grp", None, None), P("grp", None), P("grp", None, None))
    return jax.shard_map(
        body, mesh=mesh, in_specs=placed, out_specs=P(None, AXES, None), check_vma=False
    )
```

```python
import functools

import jax
import jax.numpy as jnp
from jax import lax
from jax.experimental import pallas as pl
from jax.experimental.pallas import tpu as pltpu
from jax.sharding import PartitionSpec as P

AXES = ("grp", "row")
MOVE = ("row", "grp")
F32 = jnp.float32
BF16 = jnp.bfloat16
NT = (((1,), (1,)), ((), ()))
VMEM_LIMIT = 56 * 1024 * 1024
LANES = 128
FETCHES = 8
AHEAD = 4


def own_kernel(groups, me_ref, shard_ref, length_ref, out_ref):
    tables, blocks, _ = length_ref.shape
    halves = shard_ref.shape[1] // blocks
    per_table = halves + 1
    for g in range(groups):
        k = me_ref[0] + g * (blocks // groups)
        for t in range(tables):
            for h in range(halves):
                out_ref[g, pl.ds(t * per_table + h, 1), :] = shard_ref[t, pl.ds(k * halves + h, 1), :]
            out_ref[g, pl.ds(t * per_table + halves, 1), :] = length_ref[t, pl.ds(k, 1), :]


def own_blocks(me, shard, lengths, groups):
    return pl.pallas_call(
        functools.partial(own_kernel, groups),
        out_shape=jax.ShapeDtypeStruct((groups, 8, LANES), jnp.int32),
        in_specs=[
            pl.BlockSpec(memory_space=pltpu.SMEM),
            pl.BlockSpec(memory_space=pltpu.VMEM),
            pl.BlockSpec(memory_space=pltpu.VMEM),
        ],
        out_specs=pl.BlockSpec(memory_space=pltpu.VMEM),
        cost_estimate=pl.CostEstimate(flops=2_000_000, bytes_accessed=400_000, transcendentals=0),
        name="own",
    )(me, shard, lengths)


def front_kernel(tables, blocks, groups, cap, me_ref, shard_ref, offset_ref, table_ref, out_ref,
                 key_s, off_s, by_block, list_v, held, rows, index_0, index_1, index_2, index_3,
                 table_sem, list_sem, out_sem):
    indices = (index_0, index_1, index_2, index_3)
    look = key_s.shape[0]
    halves = look // LANES
    size = table_ref.shape[1]
    me = me_ref[0]
    part = tables * size // FETCHES
    fetch = []
    for i in range(FETCHES):
        t, at = divmod(i * part, size)
        fetch.append(
            pltpu.make_async_copy(
                table_ref.at[t, pl.ds(at, part)], held.at[pl.ds(i * part, part)], table_sem.at[i]
            )
        )
    early = FETCHES // tables
    for copy in fetch[:early]:
        copy.start()
    later = lax.broadcasted_iota(jnp.int32, (look, look), 0)
    earlier = lax.broadcasted_iota(jnp.int32, (look, look), 1)
    tri = (earlier < later).astype(F32).astype(BF16)
    places = [(lax.broadcasted_iota(jnp.int32, (8, blocks), 0) + 8 * i).astype(F32) for i in range(cap // 8)]
    listed = []
    for t in range(tables):
        hit = jnp.concatenate(
            [(shard_ref[t, pl.ds(h, blocks, stride=halves), :] == me).astype(F32) for h in range(halves)], axis=1
        )
        rank = lax.dot_general(tri, hit.astype(BF16), NT, preferred_element_type=F32)
        key_s[...] = jnp.where(jnp.transpose(hit) > 0.5, rank, -1.0)
        for h in range(halves):
            off = offset_ref[pl.ds(h * tables + t, blocks, stride=halves * tables), :] + t * size
            off_s[pl.ds(h * LANES, LANES), :] = jnp.transpose(off.astype(F32))

        def step(i, accs):
            for u in range(8):
                key = key_s[pl.ds(i * 8 + u, 1), :]
                off = off_s[pl.ds(i * 8 + u, 1), :]
                accs = tuple(jnp.where(key == pos, off, acc) for acc, pos in zip(accs, places))
            return accs

        listed += lax.fori_loop(0, look // 8, step, tuple(jnp.zeros((8, blocks), F32) for _ in places))
    listed.append(jnp.zeros((LANES - tables * cap, blocks), F32))
    by_block[...] = jnp.transpose(jnp.concatenate(listed, axis=0)).astype(jnp.int32)
    tiles = blocks // groups
    for tile in range(tiles):
        list_v[pl.ds(tile * groups, groups), :] = by_block[pl.ds(tile, groups, stride=tiles), :]

    per_block = tables * cap
    per_tile = groups * per_block

    def index_copy(tile, slot):
        return pltpu.make_async_copy(list_v.at[pl.ds(tile * groups, groups)], indices[slot], list_sem.at[slot])

    def out_copy(tile):
        span = pl.ds(tile * per_tile, per_tile)
        return pltpu.make_async_copy(rows.at[span], out_ref.at[span], out_sem.at[tile])

    for slot in range(4):
        index_copy(slot, slot).start()
    for copy in fetch[early:]:
        copy.start()
    spans = 2
    fours = tiles // 4 // spans
    span_step = 4 * fours
    for span in range(spans):
        for t in range(tables):
            if span == 0:
                for copy in fetch[t * early : (t + 1) * early]:
                    copy.wait()
            last = t == tables - 1

            def four(i, carry):
                for slot in range(4):
                    tile = i * 4 + slot
                    index_copy(tile, slot).wait()
                    for u in range(groups):
                        for j in range(t * cap, (t + 1) * cap):
                            row = indices[slot][u, j]
                            rows[pl.ds(tile * per_tile + u * per_block + j, 1), :] = held[pl.ds(row, 1), :]
                    if last:
                        out_copy(tile).start()
                    again = span * span_step + slot + (span_step if last else 0)
                    ahead = jnp.where(i + 1 < (span + 1) * fours, tile + 4, again)

                    @pl.when(ahead < tiles)
                    def _():
                        index_copy(ahead, slot).start()

                return carry

            lax.fori_loop(span * fours, (span + 1) * fours, four, 0)
    for tile in range(tiles):
        out_copy(tile).wait()


def front(me, shard, offset, table, blocks, groups, cap):
    tables, size, width = table.shape
    look = shard.shape[1] * LANES // blocks
    return pl.pallas_call(
        functools.partial(front_kernel, tables, blocks, groups, cap),
        out_shape=jax.ShapeDtypeStruct((blocks * tables * cap, width), F32),
        in_specs=[
            pl.BlockSpec(memory_space=pltpu.SMEM),
            pl.BlockSpec(memory_space=pltpu.VMEM),
            pl.BlockSpec(memory_space=pltpu.VMEM),
            pl.BlockSpec(memory_space=pl.ANY),
        ],
        out_specs=pl.BlockSpec(memory_space=pl.ANY),
        scratch_shapes=[
            pltpu.VMEM((look, blocks), F32),
            pltpu.VMEM((look, blocks), F32),
            pltpu.VMEM((blocks, LANES), jnp.int32),
            pltpu.VMEM((blocks, LANES), jnp.int32),
            pltpu.VMEM((tables * size, width), F32),
            pltpu.VMEM((blocks * tables * cap, width), F32),
        ]
        + [pltpu.SMEM((groups, LANES), jnp.int32)] * 4
        + [
            pltpu.SemaphoreType.DMA((FETCHES,)),
            pltpu.SemaphoreType.DMA((4,)),
            pltpu.SemaphoreType.DMA((blocks // groups,)),
        ],
        compiler_params=pltpu.CompilerParams(vmem_limit_bytes=VMEM_LIMIT),
        cost_estimate=pl.CostEstimate(flops=60_000_000, bytes_accessed=15_000_000, transcendentals=0),
        name="front",
    )(me, shard, offset, table)


def weight_kernel(tables, look, cap, shards, about_ref, out_ref):
    bags = out_ref.shape[1]
    halves = look // LANES
    row = lax.broadcasted_iota(jnp.int32, (look, look), 0)
    col = lax.broadcasted_iota(jnp.int32, (look, look), 1)
    upper = (row < col).astype(F32).astype(BF16)
    ids = lax.broadcasted_iota(jnp.int32, (shards, look), 0).astype(F32)
    places = lax.broadcasted_iota(jnp.int32, (shards * cap, look), 0).astype(F32)
    brow = lax.broadcasted_iota(jnp.int32, (bags, bags), 0)
    bcol = lax.broadcasted_iota(jnp.int32, (bags, bags), 1)
    spot = lax.broadcasted_iota(jnp.int32, (bags, look), 1).astype(F32)
    for t in range(tables):
        first = t * (halves + 1)
        shard = jnp.concatenate(
            [about_ref[0, pl.ds(first + h, 1), :] for h in range(halves)], axis=1
        ).astype(F32)
        length = about_ref[0, pl.ds(first + halves, 1), :].astype(F32)
        hit = (shard == ids).astype(F32)
        before = jnp.dot(hit.astype(BF16), upper, preferred_element_type=F32)
        slot = jnp.sum(hit * before, axis=0, keepdims=True) + shard * cap
        chosen = (places == slot).astype(F32).astype(BF16)
        ends = jnp.sum(jnp.where(bcol <= brow, length, 0.0), axis=1, keepdims=True)
        starts = jnp.sum(jnp.where(bcol < brow, length, 0.0), axis=1, keepdims=True)
        inside = ((spot >= starts) & (spot < ends)).astype(F32).astype(BF16)
        out_ref[t] = lax.dot_general(inside, chosen, NT, preferred_element_type=F32).astype(BF16)


def make_weights(about, tables, bags, look, cap, shards):
    groups = about.shape[0]
    return pl.pallas_call(
        functools.partial(weight_kernel, tables, look, cap, shards),
        grid=(groups,),
        out_shape=jax.ShapeDtypeStruct((groups * tables, bags, shards * cap), BF16),
        in_specs=[pl.BlockSpec((1, 8, LANES), lambda i: (i, 0, 0))],
        out_specs=pl.BlockSpec((tables, bags, shards * cap), lambda i: (i, 0, 0)),
        compiler_params=pltpu.CompilerParams(vmem_limit_bytes=16 * 1024 * 1024),
        cost_estimate=pl.CostEstimate(flops=30_000_000, bytes_accessed=3_000_000, transcendentals=0),
        name="weights",
    )(about)


def pool_kernel(groups, tables, cap, weight_ref, rows_ref, out_ref, rows_v, out_v, rows_sem, out_sem):
    _, shards, _, width = rows_v.shape

    def rows_copy(g):
        return pltpu.make_async_copy(rows_ref.at[:, g], rows_v.at[g], rows_sem.at[g])

    def out_copy(g):
        span = pl.ds(g * tables, tables)
        return pltpu.make_async_copy(out_v.at[span], out_ref.at[span], out_sem.at[g])

    for g in range(AHEAD):
        rows_copy(g).start()

    def group(g, carry):
        @pl.when(g + AHEAD < groups)
        def _():
            rows_copy(g + AHEAD).start()

        rows_copy(g).wait()
        for t in range(tables):
            rows = rows_v[g, :, pl.ds(t * cap, cap), :].reshape(shards * cap, width)
            high = rows.astype(BF16)
            low = (rows - high.astype(F32)).astype(BF16)
            both = jnp.dot(
                weight_ref[g * tables + t], jnp.concatenate([high, low], axis=1), preferred_element_type=F32
            )
            out_v[g * tables + t] = both[:, :width] + both[:, width:]
        out_copy(g).start()
        return carry

    lax.fori_loop(0, groups, group, 0)
    for g in range(groups):
        out_copy(g).wait()


def pool(weights, rows, groups, cap):
    total, bags, _ = weights.shape
    shards, _, slots, width = rows.shape
    return pl.pallas_call(
        functools.partial(pool_kernel, groups, total // groups, cap),
        out_shape=jax.ShapeDtypeStruct((total, bags, width), F32),
        in_specs=[pl.BlockSpec(memory_space=pltpu.VMEM), pl.BlockSpec(memory_space=pl.ANY)],
        out_specs=pl.BlockSpec(memory_space=pl.ANY),
        scratch_shapes=[
            pltpu.VMEM((groups, shards, slots, width), F32),
            pltpu.VMEM((total, bags, width), F32),
            pltpu.SemaphoreType.DMA((groups,)),
            pltpu.SemaphoreType.DMA((groups,)),
        ],
        compiler_params=pltpu.CompilerParams(vmem_limit_bytes=40 * 1024 * 1024),
        cost_estimate=pl.CostEstimate(flops=20_000_000, bytes_accessed=4_000_000, transcendentals=0),
        name="pool",
    )(weights, rows)


def body(table, row_shard, row_offset, bag_lengths):
    groups = lax.axis_size("grp")
    shards = lax.axis_size("row")
    mine = lax.axis_index("row")
    tables, _, width = table.shape
    blocks, bags = bag_lengths.shape[1:]
    lookups = row_offset.shape[1]
    look = lookups // blocks
    cap = 3 * look // shards

    shard = row_shard.reshape(tables, lookups // LANES, LANES)
    offset = row_offset.reshape(tables, lookups // LANES, LANES).transpose(1, 0, 2)
    rows = front(mine.reshape(1), shard, offset.reshape(-1, LANES), table, blocks, groups, cap)
    moved = lax.all_to_all(rows.reshape(blocks, tables * cap, width), MOVE, 0, 0, tiled=True)
    moved = moved.reshape(shards, groups, tables * cap, width)

    own = own_blocks(mine.reshape(1), shard, bag_lengths, groups)
    about = lax.all_to_all(own, "grp", 0, 0, tiled=True)
    weights = make_weights(about, tables, bags, look, cap, shards)
    return pool(weights, moved, groups, cap)


def solution(mesh):
    placed = (P("grp", "row", None), P("grp", None, None), P("grp", None), P("grp", None, None))
    return jax.shard_map(
        body, mesh=mesh, in_specs=placed, out_specs=P(None, AXES, None), check_vma=False
    )
```

```python
import functools

import jax
import jax.numpy as jnp
from jax import lax
from jax.experimental import pallas as pl
from jax.experimental.pallas import tpu as pltpu
from jax.sharding import PartitionSpec as P

AXES = ("grp", "row")
MOVE = ("row", "grp")
F32 = jnp.float32
BF16 = jnp.bfloat16
NT = (((1,), (1,)), ((), ()))
VMEM_LIMIT = 56 * 1024 * 1024
LANES = 128
FETCHES = 8


def front_kernel(tables, blocks, groups, cap, me_ref, shard_ref, offset_ref, length_ref, table_ref, out_ref,
                 key_s, off_s, end_s, by_block, meta_v, list_v, held, rows, index_0, index_1, index_2, index_3,
                 table_sem, list_sem, out_sem):
    indices = (index_0, index_1, index_2, index_3)
    look = key_s.shape[0]
    halves = look // LANES
    size = table_ref.shape[1]
    me = me_ref[0]
    part = tables * size // FETCHES
    fetch = []
    for i in range(FETCHES):
        t, at = divmod(i * part, size)
        fetch.append(
            pltpu.make_async_copy(
                table_ref.at[t, pl.ds(at, part)], held.at[pl.ds(i * part, part)], table_sem.at[i]
            )
        )
    early = FETCHES // tables
    for copy in fetch[:early]:
        copy.start()
    later = lax.broadcasted_iota(jnp.int32, (look, look), 0)
    earlier = lax.broadcasted_iota(jnp.int32, (look, look), 1)
    tri = (earlier < later).astype(F32).astype(BF16)
    places = [(lax.broadcasted_iota(jnp.int32, (8, blocks), 0) + 8 * i).astype(F32) for i in range(cap // 8)]
    bags = length_ref.shape[2]
    upto = lax.broadcasted_iota(jnp.int32, (bags, bags), 1) <= lax.broadcasted_iota(jnp.int32, (bags, bags), 0)
    upto = upto.astype(F32).astype(BF16)
    lane = lax.broadcasted_iota(jnp.int32, (blocks, LANES), 1)
    listed, bag_of = [], []
    for t in range(tables):
        hit = jnp.concatenate(
            [(shard_ref[t, pl.ds(h, blocks, stride=halves), :] == me).astype(F32) for h in range(halves)], axis=1
        )
        rank = lax.dot_general(tri, hit.astype(BF16), NT, preferred_element_type=F32)
        key_s[...] = jnp.where(jnp.transpose(hit) > 0.5, rank, -1.0)
        for h in range(halves):
            off = offset_ref[pl.ds(h * tables + t, blocks, stride=halves * tables), :] + t * size
            packed = off * look + (lane + h * LANES)
            off_s[pl.ds(h * LANES, LANES), :] = jnp.transpose(packed.astype(F32))
        end_s[...] = lax.dot_general(
            upto, length_ref[t].astype(F32).astype(BF16), NT, preferred_element_type=F32
        )

        def step(i, accs):
            for u in range(8):
                key = key_s[pl.ds(i * 8 + u, 1), :]
                off = off_s[pl.ds(i * 8 + u, 1), :]
                accs = tuple(jnp.where(key == pos, off, acc) for acc, pos in zip(accs, places))
            return accs

        found = lax.fori_loop(0, look // 8, step, tuple(jnp.full((8, blocks), -1.0, F32) for _ in places))
        found = [value.astype(jnp.int32) for value in found]
        spots = [(value & (look - 1)).astype(F32) for value in found]

        def count(i, accs):
            for u in range(8):
                end = end_s[pl.ds(i * 8 + u, 1), :]
                accs = tuple(acc + jnp.where(end <= spot, 1.0, 0.0) for acc, spot in zip(accs, spots))
            return accs

        counts = lax.fori_loop(0, bags // 8, count, tuple(jnp.zeros((8, blocks), F32) for _ in places))
        listed += [(jnp.maximum(value, 0) // look).astype(F32) for value in found]
        bag_of += [jnp.where(value >= 0, number, -1.0) for value, number in zip(found, counts)]
    spare = jnp.full((LANES - tables * cap, blocks), -1.0, F32)
    by_block[...] = jnp.transpose(jnp.concatenate(listed + [spare], axis=0)).astype(jnp.int32)
    turned = jnp.transpose(jnp.concatenate(bag_of + [spare], axis=0))
    meta_v[...] = pltpu.roll(turned, lax.rem(me * cap, LANES), 1)
    tiles = blocks // groups
    for tile in range(tiles):
        list_v[pl.ds(tile * groups, groups), :] = by_block[pl.ds(tile, groups, stride=tiles), :]
    per_block = tables * cap + 1
    per_tile = groups * per_block
    for tile in range(tiles):
        last_rows = pl.ds(tile * per_tile + per_block - 1, groups, stride=per_block)
        rows[last_rows, :] = meta_v[pl.ds(tile, groups, stride=tiles), :]

    def index_copy(tile, slot):
        return pltpu.make_async_copy(list_v.at[pl.ds(tile * groups, groups)], indices[slot], list_sem.at[slot])

    def out_copy(tile):
        span = pl.ds(tile * per_tile, per_tile)
        return pltpu.make_async_copy(rows.at[span], out_ref.at[span], out_sem.at[tile])

    for slot in range(4):
        index_copy(slot, slot).start()
    for copy in fetch[early:]:
        copy.start()
    spans = 2
    fours = tiles // 4 // spans
    span_step = 4 * fours
    for span in range(spans):
        for t in range(tables):
            if span == 0:
                for copy in fetch[t * early : (t + 1) * early]:
                    copy.wait()
            last = t == tables - 1

            def four(i, carry):
                for slot in range(4):
                    tile = i * 4 + slot
                    index_copy(tile, slot).wait()
                    for u in range(groups):
                        for j in range(t * cap, (t + 1) * cap):
                            row = indices[slot][u, j]
                            rows[pl.ds(tile * per_tile + u * per_block + j, 1), :] = held[pl.ds(row, 1), :]
                    if last:
                        out_copy(tile).start()
                    again = span * span_step + slot + (span_step if last else 0)
                    ahead = jnp.where(i + 1 < (span + 1) * fours, tile + 4, again)

                    @pl.when(ahead < tiles)
                    def _():
                        index_copy(ahead, slot).start()

                return carry

            lax.fori_loop(span * fours, (span + 1) * fours, four, 0)
    for tile in range(tiles):
        out_copy(tile).wait()


def front(me, shard, offset, lengths, table, blocks, groups, cap):
    tables, size, width = table.shape
    count = blocks * (tables * cap + 1)
    look = shard.shape[1] * LANES // blocks
    return pl.pallas_call(
        functools.partial(front_kernel, tables, blocks, groups, cap),
        out_shape=jax.ShapeDtypeStruct((count, width), F32),
        in_specs=[
            pl.BlockSpec(memory_space=pltpu.SMEM),
            pl.BlockSpec(memory_space=pltpu.VMEM),
            pl.BlockSpec(memory_space=pltpu.VMEM),
            pl.BlockSpec(memory_space=pltpu.VMEM),
            pl.BlockSpec(memory_space=pl.ANY),
        ],
        out_specs=pl.BlockSpec(memory_space=pl.ANY),
        scratch_shapes=[
            pltpu.VMEM((look, blocks), F32),
            pltpu.VMEM((look, blocks), F32),
            pltpu.VMEM((lengths.shape[2], blocks), F32),
            pltpu.VMEM((blocks, LANES), jnp.int32),
            pltpu.VMEM((blocks, LANES), F32),
            pltpu.VMEM((blocks, LANES), jnp.int32),
            pltpu.VMEM((tables * size, width), F32),
            pltpu.VMEM((count, width), F32),
        ]
        + [pltpu.SMEM((groups, LANES), jnp.int32)] * 4
        + [
            pltpu.SemaphoreType.DMA((FETCHES,)),
            pltpu.SemaphoreType.DMA((4,)),
            pltpu.SemaphoreType.DMA((blocks // groups,)),
        ],
        compiler_params=pltpu.CompilerParams(vmem_limit_bytes=VMEM_LIMIT),
        cost_estimate=pl.CostEstimate(flops=60_000_000, bytes_accessed=15_000_000, transcendentals=0),
        name="front",
    )(me, shard, offset, lengths, table)


def pool_kernel(groups, shards, tables, cap, rows_ref, out_ref, rows_v, out_v, rows_sem, out_sem):
    bags = out_v.shape[1]
    width = rows_v.shape[1]
    per_block = tables * cap + 1
    part = 2 * (per_block - 1) + 8

    def rows_copy(q, s):
        source = pl.ds((s * groups) * per_block + 2 * (per_block - 1) * q, part)
        target = pl.ds((q * shards + s) * part, part)
        return pltpu.make_async_copy(rows_ref.at[source], rows_v.at[target], rows_sem.at[q, s])

    def out_copy(g):
        span = pl.ds(g * tables, tables)
        return pltpu.make_async_copy(out_v.at[span], out_ref.at[span], out_sem.at[g])

    for q in range(groups // 2):
        for s in range(shards):
            rows_copy(q, s).start()
    numbers = lax.broadcasted_iota(jnp.int32, (bags, LANES), 0).astype(F32)
    lane = lax.broadcasted_iota(jnp.int32, (1, LANES), 1)
    for q in range(groups // 2):
        for s in range(shards):
            rows_copy(q, s).wait()

        def group(i, carry):
            g = 2 * q + i
            first = 2 * q + i * per_block
            start = q * shards * part + first
            meta = rows_v[pl.ds(start + per_block - 1, shards, stride=part), :]
            for t in range(tables):
                turned = meta if t == 0 else pltpu.roll(meta, LANES - t * cap, 1)
                weight = []
                for v in range(shards * cap // LANES):
                    low = v * LANES // cap
                    high = ((v + 1) * LANES - 1) // cap
                    bag = turned[low : low + 1, :]
                    for s in range(low + 1, high + 1):
                        bag = jnp.where(lane >= s * cap - v * LANES, turned[s : s + 1, :], bag)
                    weight.append((bag == numbers).astype(F32).astype(BF16))
                rows = jnp.concatenate(
                    [rows_v[pl.ds(start + s * part + t * cap, cap), :] for s in range(shards)], axis=0
                )
                high_part = rows.astype(BF16)
                low_part = (rows - high_part.astype(F32)).astype(BF16)
                both = jnp.dot(
                    jnp.concatenate(weight, axis=1),
                    jnp.concatenate([high_part, low_part], axis=1),
                    preferred_element_type=F32,
                )
                out_v[g * tables + t] = both[:, :width] + both[:, width:]
            out_copy(g).start()
            return carry

        lax.fori_loop(0, 2, group, 0)
    for g in range(groups):
        out_copy(g).wait()


def pool(rows, groups, shards, tables, bags, cap):
    width = rows.shape[1]
    part = 2 * tables * cap + 8
    return pl.pallas_call(
        functools.partial(pool_kernel, groups, shards, tables, cap),
        out_shape=jax.ShapeDtypeStruct((groups * tables, bags, width), F32),
        in_specs=[pl.BlockSpec(memory_space=pl.ANY)],
        out_specs=pl.BlockSpec(memory_space=pl.ANY),
        scratch_shapes=[
            pltpu.VMEM((groups // 2 * shards * part, width), F32),
            pltpu.VMEM((groups * tables, bags, width), F32),
            pltpu.SemaphoreType.DMA((groups // 2, shards)),
            pltpu.SemaphoreType.DMA((groups,)),
        ],
        compiler_params=pltpu.CompilerParams(vmem_limit_bytes=VMEM_LIMIT),
        cost_estimate=pl.CostEstimate(flops=20_000_000, bytes_accessed=8_000_000, transcendentals=0),
        name="pool",
    )(rows)


def body(table, row_shard, row_offset, bag_lengths):
    groups = lax.axis_size("grp")
    shards = lax.axis_size("row")
    mine = lax.axis_index("row")
    tables, _, width = table.shape
    blocks, bags = bag_lengths.shape[1:]
    lookups = row_offset.shape[1]
    look = lookups // blocks
    cap = 3 * look // shards

    shard = row_shard.reshape(tables, lookups // LANES, LANES)
    offset = row_offset.reshape(tables, lookups // LANES, LANES).transpose(1, 0, 2)
    offset = offset.reshape(-1, LANES)
    rows = front(mine.reshape(1), shard, offset, bag_lengths, table, blocks, groups, cap)
    moved = lax.all_to_all(rows.reshape(blocks, tables * cap + 1, 1, width), MOVE, 0, 0, tiled=True)
    return pool(moved.reshape(-1, width), groups, shards, tables, bags, cap)


def solution(mesh):
    placed = (P("grp", "row", None), P("grp", None, None), P("grp", None), P("grp", None, None))
    return jax.shard_map(
        body, mesh=mesh, in_specs=placed, out_specs=P(None, AXES, None), check_vma=False
    )
```

```python
import functools

import jax
import jax.numpy as jnp
from jax import lax
from jax.experimental import pallas as pl
from jax.experimental.pallas import tpu as pltpu
from jax.sharding import PartitionSpec as P

AXES = ("grp", "row")
MOVE = ("row", "grp")
F32 = jnp.float32
BF16 = jnp.bfloat16
NT = (((1,), (1,)), ((), ()))
VMEM_LIMIT = 56 * 1024 * 1024
LANES = 128
FETCHES = 8


def front_kernel(tables, blocks, groups, cap, me_ref, shard_ref, offset_ref, length_ref, table_ref, out_ref,
                 key_s, off_s, end_s, by_block, meta_v, list_v, held, rows, index_0, index_1, index_2, index_3,
                 table_sem, list_sem, out_sem):
    indices = (index_0, index_1, index_2, index_3)
    look = key_s.shape[0]
    halves = look // LANES
    size = table_ref.shape[1]
    me = me_ref[0]
    part = tables * size // FETCHES
    fetch = []
    for i in range(FETCHES):
        t, at = divmod(i * part, size)
        fetch.append(
            pltpu.make_async_copy(
                table_ref.at[t, pl.ds(at, part)], held.at[pl.ds(i * part, part)], table_sem.at[i]
            )
        )
    early = FETCHES // tables
    for copy in fetch[:early]:
        copy.start()
    later = lax.broadcasted_iota(jnp.int32, (look, look), 0)
    earlier = lax.broadcasted_iota(jnp.int32, (look, look), 1)
    tri = (earlier < later).astype(F32).astype(BF16)
    places = [(lax.broadcasted_iota(jnp.int32, (8, blocks), 0) + 8 * i).astype(F32) for i in range(cap // 8)]
    bags = length_ref.shape[2]
    upto = lax.broadcasted_iota(jnp.int32, (bags, bags), 1) <= lax.broadcasted_iota(jnp.int32, (bags, bags), 0)
    upto = upto.astype(F32).astype(BF16)
    lane = lax.broadcasted_iota(jnp.int32, (blocks, LANES), 1)
    tiles = blocks // groups
    bag_of = []

    def index_copy(t, tile, slot):
        source = list_v.at[pl.ds(t * blocks + tile * groups, groups)]
        return pltpu.make_async_copy(source, indices[slot], list_sem.at[slot])

    for t in range(tables):
        hit = jnp.concatenate(
            [(shard_ref[t, pl.ds(h, blocks, stride=halves), :] == me).astype(F32) for h in range(halves)], axis=1
        )
        rank = lax.dot_general(tri, hit.astype(BF16), NT, preferred_element_type=F32)
        key_s[...] = jnp.where(jnp.transpose(hit) > 0.5, rank, -1.0)
        for h in range(halves):
            off = offset_ref[pl.ds(h * tables + t, blocks, stride=halves * tables), :] + t * size
            packed = off * look + (lane + h * LANES)
            off_s[pl.ds(h * LANES, LANES), :] = jnp.transpose(packed.astype(F32))
        end_s[...] = lax.dot_general(
            upto, length_ref[t].astype(F32).astype(BF16), NT, preferred_element_type=F32
        )

        def step(i, accs):
            for u in range(8):
                key = key_s[pl.ds(i * 8 + u, 1), :]
                off = off_s[pl.ds(i * 8 + u, 1), :]
                accs = tuple(jnp.where(key == pos, off, acc) for acc, pos in zip(accs, places))
            return accs

        found = lax.fori_loop(0, look // 8, step, tuple(jnp.full((8, blocks), -1.0, F32) for _ in places))
        found = [value.astype(jnp.int32) for value in found]
        spots = [(value & (look - 1)).astype(F32) for value in found]

        spare = jnp.full((LANES - cap, blocks), -1.0, F32)
        listed = [(jnp.maximum(value, 0) // look).astype(F32) for value in found]
        by_block[...] = jnp.transpose(jnp.concatenate(listed + [spare], axis=0)).astype(jnp.int32)
        for tile in range(tiles):
            to = pl.ds(t * blocks + tile * groups, groups)
            list_v[to, :] = by_block[pl.ds(tile, groups, stride=tiles), :]
        if t == 0:
            for slot in range(4):
                index_copy(0, slot, slot).start()
            for copy in fetch[early:]:
                copy.start()

        def count(i, accs):
            for u in range(8):
                end = end_s[pl.ds(i * 8 + u, 1), :]
                accs = tuple(acc + jnp.where(end <= spot, 1.0, 0.0) for acc, spot in zip(accs, spots))
            return accs

        counts = lax.fori_loop(0, bags // 8, count, tuple(jnp.zeros((8, blocks), F32) for _ in places))
        bag_of += [jnp.where(value >= 0, number, -1.0) for value, number in zip(found, counts)]
    spare = jnp.full((LANES - tables * cap, blocks), -1.0, F32)
    turned = jnp.transpose(jnp.concatenate(bag_of + [spare], axis=0))
    meta_v[...] = pltpu.roll(turned, lax.rem(me * cap, LANES), 1)
    per_block = tables * cap + 1
    per_tile = groups * per_block
    for tile in range(tiles):
        last_rows = pl.ds(tile * per_tile + per_block - 1, groups, stride=per_block)
        rows[last_rows, :] = meta_v[pl.ds(tile, groups, stride=tiles), :]

    def out_copy(tile):
        span = pl.ds(tile * per_tile, per_tile)
        return pltpu.make_async_copy(rows.at[span], out_ref.at[span], out_sem.at[tile])

    spans = 2
    fours = tiles // 4 // spans
    span_step = 4 * fours
    for span in range(spans):
        for t in range(tables):
            if span == 0:
                for copy in fetch[t * early : (t + 1) * early]:
                    copy.wait()
            last = t == tables - 1

            def four(i, carry):
                for slot in range(4):
                    tile = i * 4 + slot
                    index_copy(t, tile, slot).wait()
                    for u in range(groups):
                        for j in range(cap):
                            row = indices[slot][u, j]
                            at = tile * per_tile + u * per_block + t * cap + j
                            rows[pl.ds(at, 1), :] = held[pl.ds(row, 1), :]
                    if last:
                        out_copy(tile).start()
                    inside = i + 1 < (span + 1) * fours
                    again = span * span_step + slot + (span_step if last else 0)
                    ahead = jnp.where(inside, tile + 4, again)
                    table_ahead = jnp.where(inside, t, (t + 1) % tables)

                    @pl.when(ahead < tiles)
                    def _():
                        index_copy(table_ahead, ahead, slot).start()

                return carry

            lax.fori_loop(span * fours, (span + 1) * fours, four, 0)
    for tile in range(tiles):
        out_copy(tile).wait()


def front(me, shard, offset, lengths, table, blocks, groups, cap):
    tables, size, width = table.shape
    count = blocks * (tables * cap + 1)
    look = shard.shape[1] * LANES // blocks
    return pl.pallas_call(
        functools.partial(front_kernel, tables, blocks, groups, cap),
        out_shape=jax.ShapeDtypeStruct((count, width), F32),
        in_specs=[
            pl.BlockSpec(memory_space=pltpu.SMEM),
            pl.BlockSpec(memory_space=pltpu.VMEM),
            pl.BlockSpec(memory_space=pltpu.VMEM),
            pl.BlockSpec(memory_space=pltpu.VMEM),
            pl.BlockSpec(memory_space=pl.ANY),
        ],
        out_specs=pl.BlockSpec(memory_space=pl.ANY),
        scratch_shapes=[
            pltpu.VMEM((look, blocks), F32),
            pltpu.VMEM((look, blocks), F32),
            pltpu.VMEM((lengths.shape[2], blocks), F32),
            pltpu.VMEM((blocks, LANES), jnp.int32),
            pltpu.VMEM((blocks, LANES), F32),
            pltpu.VMEM((tables * blocks, LANES), jnp.int32),
            pltpu.VMEM((tables * size, width), F32),
            pltpu.VMEM((count, width), F32),
        ]
        + [pltpu.SMEM((groups, LANES), jnp.int32)] * 4
        + [
            pltpu.SemaphoreType.DMA((FETCHES,)),
            pltpu.SemaphoreType.DMA((4,)),
            pltpu.SemaphoreType.DMA((blocks // groups,)),
        ],
        compiler_params=pltpu.CompilerParams(vmem_limit_bytes=VMEM_LIMIT),
        cost_estimate=pl.CostEstimate(flops=60_000_000, bytes_accessed=15_000_000, transcendentals=0),
        name="front",
    )(me, shard, offset, lengths, table)


def pool_kernel(groups, shards, tables, cap, rows_ref, out_ref, rows_v, out_v, rows_sem, out_sem):
    bags = out_v.shape[1]
    width = rows_v.shape[1]
    per_block = tables * cap + 1
    part = 2 * (per_block - 1) + 8

    def rows_copy(q, s):
        source = pl.ds((s * groups) * per_block + 2 * (per_block - 1) * q, part)
        target = pl.ds((q * shards + s) * part, part)
        return pltpu.make_async_copy(rows_ref.at[source], rows_v.at[target], rows_sem.at[q, s])

    def out_copy(g):
        span = pl.ds(g * tables, tables)
        return pltpu.make_async_copy(out_v.at[span], out_ref.at[span], out_sem.at[g])

    for q in range(2):
        for s in range(shards):
            rows_copy(q, s).start()
    numbers = lax.broadcasted_iota(jnp.int32, (bags, LANES), 0).astype(F32)
    lane = lax.broadcasted_iota(jnp.int32, (1, LANES), 1)
    for q in range(groups // 2):
        for s in range(shards):
            rows_copy(q, s).wait()
        if q + 2 < groups // 2:
            for s in range(shards):
                rows_copy(q + 2, s).start()

        def group(i, carry):
            g = 2 * q + i
            first = 2 * q + i * per_block
            start = q * shards * part + first
            meta = rows_v[pl.ds(start + per_block - 1, shards, stride=part), :]
            for t in range(tables):
                turned = meta if t == 0 else pltpu.roll(meta, LANES - t * cap, 1)
                weight = []
                for v in range(shards * cap // LANES):
                    low = v * LANES // cap
                    high = ((v + 1) * LANES - 1) // cap
                    bag = turned[low : low + 1, :]
                    for s in range(low + 1, high + 1):
                        bag = jnp.where(lane >= s * cap - v * LANES, turned[s : s + 1, :], bag)
                    weight.append((bag == numbers).astype(F32).astype(BF16))
                rows = jnp.concatenate(
                    [rows_v[pl.ds(start + s * part + t * cap, cap), :] for s in range(shards)], axis=0
                )
                high_part = rows.astype(BF16)
                low_part = (rows - high_part.astype(F32)).astype(BF16)
                both = jnp.dot(
                    jnp.concatenate(weight, axis=1),
                    jnp.concatenate([high_part, low_part], axis=1),
                    preferred_element_type=F32,
                )
                out_v[g * tables + t] = both[:, :width] + both[:, width:]
            out_copy(g).start()
            return carry

        lax.fori_loop(0, 2, group, 0)
    for g in range(groups):
        out_copy(g).wait()


def pool(rows, groups, shards, tables, bags, cap):
    width = rows.shape[1]
    part = 2 * tables * cap + 8
    return pl.pallas_call(
        functools.partial(pool_kernel, groups, shards, tables, cap),
        out_shape=jax.ShapeDtypeStruct((groups * tables, bags, width), F32),
        in_specs=[pl.BlockSpec(memory_space=pl.ANY)],
        out_specs=pl.BlockSpec(memory_space=pl.ANY),
        scratch_shapes=[
            pltpu.VMEM((groups // 2 * shards * part, width), F32),
            pltpu.VMEM((groups * tables, bags, width), F32),
            pltpu.SemaphoreType.DMA((groups // 2, shards)),
            pltpu.SemaphoreType.DMA((groups,)),
        ],
        compiler_params=pltpu.CompilerParams(vmem_limit_bytes=VMEM_LIMIT),
        cost_estimate=pl.CostEstimate(flops=20_000_000, bytes_accessed=8_000_000, transcendentals=0),
        name="pool",
    )(rows)


def body(table, row_shard, row_offset, bag_lengths):
    groups = lax.axis_size("grp")
    shards = lax.axis_size("row")
    mine = lax.axis_index("row")
    tables, _, width = table.shape
    blocks, bags = bag_lengths.shape[1:]
    lookups = row_offset.shape[1]
    look = lookups // blocks
    cap = 3 * look // shards

    shard = row_shard.reshape(tables, lookups // LANES, LANES)
    offset = row_offset.reshape(tables, lookups // LANES, LANES).transpose(1, 0, 2)
    offset = offset.reshape(-1, LANES)
    rows = front(mine.reshape(1), shard, offset, bag_lengths, table, blocks, groups, cap)
    moved = lax.all_to_all(rows.reshape(blocks, tables * cap + 1, 1, width), MOVE, 0, 0, tiled=True)
    return pool(moved.reshape(-1, width), groups, shards, tables, bags, cap)


def solution(mesh):
    placed = (P("grp", "row", None), P("grp", None, None), P("grp", None), P("grp", None, None))
    return jax.shard_map(
        body, mesh=mesh, in_specs=placed, out_specs=P(None, AXES, None), check_vma=False
    )
```

```python
import functools

import jax
import jax.numpy as jnp
from jax import lax
from jax.experimental import pallas as pl
from jax.experimental.pallas import tpu as pltpu
from jax.sharding import PartitionSpec as P

AXES = ("grp", "row")
MOVE = ("row", "grp")
F32 = jnp.float32
BF16 = jnp.bfloat16
NT = (((1,), (1,)), ((), ()))
VMEM_LIMIT = 56 * 1024 * 1024
LANES = 128
FETCHES = 8
SLOTS = 8


def front_kernel(tables, blocks, groups, cap, me_ref, shard_ref, offset_ref, length_ref, table_ref, out_ref,
                 key_s, off_s, end_s, by_block, meta_v, list_v, held, rows, *rest):
    indices, (table_sem, list_sem, out_sem) = rest[:SLOTS], rest[SLOTS:]
    look = key_s.shape[0]
    halves = look // LANES
    size = table_ref.shape[1]
    me = me_ref[0]
    part = tables * size // FETCHES
    fetch = []
    for i in range(FETCHES):
        t, at = divmod(i * part, size)
        fetch.append(
            pltpu.make_async_copy(
                table_ref.at[t, pl.ds(at, part)], held.at[pl.ds(i * part, part)], table_sem.at[i]
            )
        )
    early = FETCHES // tables
    for copy in fetch[:early]:
        copy.start()
    later = lax.broadcasted_iota(jnp.int32, (look, look), 0)
    earlier = lax.broadcasted_iota(jnp.int32, (look, look), 1)
    tri = (earlier < later).astype(F32).astype(BF16)
    places = [(lax.broadcasted_iota(jnp.int32, (8, blocks), 0) + 8 * i).astype(F32) for i in range(cap // 8)]
    bags = length_ref.shape[2]
    upto = lax.broadcasted_iota(jnp.int32, (bags, bags), 1) <= lax.broadcasted_iota(jnp.int32, (bags, bags), 0)
    upto = upto.astype(F32).astype(BF16)
    lane = lax.broadcasted_iota(jnp.int32, (blocks, LANES), 1)
    tiles = blocks // groups
    bag_of = []

    def index_copy(t, tile, slot):
        source = list_v.at[pl.ds(t * blocks + tile * groups, groups)]
        return pltpu.make_async_copy(source, indices[slot], list_sem.at[slot])

    for t in range(tables):
        hit = jnp.concatenate(
            [(shard_ref[t, pl.ds(h, blocks, stride=halves), :] == me).astype(F32) for h in range(halves)], axis=1
        )
        rank = lax.dot_general(tri, hit.astype(BF16), NT, preferred_element_type=F32)
        key_s[...] = jnp.where(jnp.transpose(hit) > 0.5, rank, -1.0)
        for h in range(halves):
            off = offset_ref[pl.ds(h * tables + t, blocks, stride=halves * tables), :] + t * size
            packed = off * look + (lane + h * LANES)
            off_s[pl.ds(h * LANES, LANES), :] = jnp.transpose(packed.astype(F32))
        end_s[...] = lax.dot_general(
            upto, length_ref[t].astype(F32).astype(BF16), NT, preferred_element_type=F32
        )

        def step(i, accs):
            for u in range(8):
                key = key_s[pl.ds(i * 8 + u, 1), :]
                off = off_s[pl.ds(i * 8 + u, 1), :]
                accs = tuple(jnp.where(key == pos, off, acc) for acc, pos in zip(accs, places))
            return accs

        found = lax.fori_loop(0, look // 8, step, tuple(jnp.full((8, blocks), -1.0, F32) for _ in places))
        found = [value.astype(jnp.int32) for value in found]
        spots = [(value & (look - 1)).astype(F32) for value in found]

        spare = jnp.full((LANES - cap, blocks), -1.0, F32)
        listed = [(jnp.maximum(value, 0) // look).astype(F32) for value in found]
        by_block[...] = jnp.transpose(jnp.concatenate(listed + [spare], axis=0)).astype(jnp.int32)
        for tile in range(tiles):
            to = pl.ds(t * blocks + tile * groups, groups)
            list_v[to, :] = by_block[pl.ds(tile, groups, stride=tiles), :]
        if t == 0:
            for slot in range(SLOTS):
                index_copy(0, slot, slot).start()
            for copy in fetch[early:]:
                copy.start()

        def count(i, accs):
            for u in range(8):
                end = end_s[pl.ds(i * 8 + u, 1), :]
                accs = tuple(acc + jnp.where(end <= spot, 1.0, 0.0) for acc, spot in zip(accs, spots))
            return accs

        counts = lax.fori_loop(0, bags // 8, count, tuple(jnp.zeros((8, blocks), F32) for _ in places))
        bag_of += [jnp.where(value >= 0, number, -1.0) for value, number in zip(found, counts)]
    spare = jnp.full((LANES - tables * cap, blocks), -1.0, F32)
    turned = jnp.transpose(jnp.concatenate(bag_of + [spare], axis=0))
    meta_v[...] = pltpu.roll(turned, lax.rem(me * cap, LANES), 1)
    per_block = tables * cap + 1
    per_tile = groups * per_block
    for tile in range(tiles):
        last_rows = pl.ds(tile * per_tile + per_block - 1, groups, stride=per_block)
        rows[last_rows, :] = meta_v[pl.ds(tile, groups, stride=tiles), :]

    def out_copy(tile):
        span = pl.ds(tile * per_tile, per_tile)
        return pltpu.make_async_copy(rows.at[span], out_ref.at[span], out_sem.at[tile])

    rounds = tiles // SLOTS
    for t in range(tables):
        for copy in fetch[t * early : (t + 1) * early]:
            copy.wait()
        last = t == tables - 1

        def several(i, carry):
            for slot in range(SLOTS):
                tile = i * SLOTS + slot
                index_copy(t, tile, slot).wait()
                for u in range(groups):
                    for j in range(cap):
                        row = indices[slot][u, j]
                        at = tile * per_tile + u * per_block + t * cap + j
                        rows[pl.ds(at, 1), :] = held[pl.ds(row, 1), :]
                if last:
                    out_copy(tile).start()
                inside = i + 1 < rounds

                @pl.when(inside)
                def _():
                    index_copy(t, tile + SLOTS, slot).start()

                if not last:

                    @pl.when(jnp.logical_not(inside))
                    def _():
                        index_copy(t + 1, slot, slot).start()

            return carry

        lax.fori_loop(0, rounds, several, 0)
    for tile in range(tiles):
        out_copy(tile).wait()


def front(me, shard, offset, lengths, table, blocks, groups, cap):
    tables, size, width = table.shape
    count = blocks * (tables * cap + 1)
    look = shard.shape[1] * LANES // blocks
    return pl.pallas_call(
        functools.partial(front_kernel, tables, blocks, groups, cap),
        out_shape=jax.ShapeDtypeStruct((count, width), F32),
        in_specs=[
            pl.BlockSpec(memory_space=pltpu.SMEM),
            pl.BlockSpec(memory_space=pltpu.VMEM),
            pl.BlockSpec(memory_space=pltpu.VMEM),
            pl.BlockSpec(memory_space=pltpu.VMEM),
            pl.BlockSpec(memory_space=pl.ANY),
        ],
        out_specs=pl.BlockSpec(memory_space=pl.ANY),
        scratch_shapes=[
            pltpu.VMEM((look, blocks), F32),
            pltpu.VMEM((look, blocks), F32),
            pltpu.VMEM((lengths.shape[2], blocks), F32),
            pltpu.VMEM((blocks, LANES), jnp.int32),
            pltpu.VMEM((blocks, LANES), F32),
            pltpu.VMEM((tables * blocks, LANES), jnp.int32),
            pltpu.VMEM((tables * size, width), F32),
            pltpu.VMEM((count, width), F32),
        ]
        + [pltpu.SMEM((groups, LANES), jnp.int32)] * SLOTS
        + [
            pltpu.SemaphoreType.DMA((FETCHES,)),
            pltpu.SemaphoreType.DMA((SLOTS,)),
            pltpu.SemaphoreType.DMA((blocks // groups,)),
        ],
        compiler_params=pltpu.CompilerParams(vmem_limit_bytes=VMEM_LIMIT),
        cost_estimate=pl.CostEstimate(flops=60_000_000, bytes_accessed=15_000_000, transcendentals=0),
        name="front",
    )(me, shard, offset, lengths, table)


def pool_kernel(groups, shards, tables, cap, rows_ref, out_ref, out_v, out_sem):
    bags = out_v.shape[1]
    width = rows_ref.shape[1]
    per_block = tables * cap + 1
    step = groups * per_block

    def out_copy(g):
        span = pl.ds(g * tables, tables)
        return pltpu.make_async_copy(out_v.at[span], out_ref.at[span], out_sem.at[g])

    numbers = lax.broadcasted_iota(jnp.int32, (bags, LANES), 0).astype(F32)
    lane = lax.broadcasted_iota(jnp.int32, (1, LANES), 1)

    def group(g, carry):
        start = g * per_block
        meta = rows_ref[pl.ds(start + per_block - 1, shards, stride=step), :]
        for t in range(tables):
            turned = meta if t == 0 else pltpu.roll(meta, LANES - t * cap, 1)
            weight = []
            for v in range(shards * cap // LANES):
                low = v * LANES // cap
                high = ((v + 1) * LANES - 1) // cap
                bag = turned[low : low + 1, :]
                for s in range(low + 1, high + 1):
                    bag = jnp.where(lane >= s * cap - v * LANES, turned[s : s + 1, :], bag)
                weight.append((bag == numbers).astype(F32).astype(BF16))
            rows = jnp.concatenate(
                [rows_ref[pl.ds(start + s * step + t * cap, cap), :] for s in range(shards)], axis=0
            )
            high_part = rows.astype(BF16)
            low_part = (rows - high_part.astype(F32)).astype(BF16)
            both = jnp.dot(
                jnp.concatenate(weight, axis=1),
                jnp.concatenate([high_part, low_part], axis=1),
                preferred_element_type=F32,
            )
            out_v[g * tables + t] = both[:, :width] + both[:, width:]
        out_copy(g).start()
        return carry

    lax.fori_loop(0, groups, group, 0)
    for g in range(groups):
        out_copy(g).wait()


def pool(rows, groups, shards, tables, bags, cap):
    width = rows.shape[1]
    return pl.pallas_call(
        functools.partial(pool_kernel, groups, shards, tables, cap),
        out_shape=jax.ShapeDtypeStruct((groups * tables, bags, width), F32),
        in_specs=[pl.BlockSpec(memory_space=pltpu.VMEM)],
        out_specs=pl.BlockSpec(memory_space=pl.ANY),
        scratch_shapes=[
            pltpu.VMEM((groups * tables, bags, width), F32),
            pltpu.SemaphoreType.DMA((groups,)),
        ],
        compiler_params=pltpu.CompilerParams(vmem_limit_bytes=16 * 1024 * 1024),
        cost_estimate=pl.CostEstimate(flops=20_000_000, bytes_accessed=8_000_000, transcendentals=0),
        name="pool",
    )(rows)


def body(table, row_shard, row_offset, bag_lengths):
    groups = lax.axis_size("grp")
    shards = lax.axis_size("row")
    mine = lax.axis_index("row")
    tables, _, width = table.shape
    blocks, bags = bag_lengths.shape[1:]
    lookups = row_offset.shape[1]
    look = lookups // blocks
    cap = 3 * look // shards

    shard = row_shard.reshape(tables, lookups // LANES, LANES)
    offset = row_offset.reshape(tables, lookups // LANES, LANES).transpose(1, 0, 2)
    offset = offset.reshape(-1, LANES)
    rows = front(mine.reshape(1), shard, offset, bag_lengths, table, blocks, groups, cap)
    moved = lax.all_to_all(rows.reshape(blocks, tables * cap + 1, 1, width), MOVE, 0, 0, tiled=True)
    return pool(moved.reshape(-1, width), groups, shards, tables, bags, cap)


def solution(mesh):
    placed = (P("grp", "row", None), P("grp", None, None), P("grp", None), P("grp", None, None))
    return jax.shard_map(
        body, mesh=mesh, in_specs=placed, out_specs=P(None, AXES, None), check_vma=False
    )
```

```python
import functools

import jax
import jax.numpy as jnp
from jax import lax
from jax.experimental import pallas as pl
from jax.experimental.pallas import tpu as pltpu
from jax.sharding import PartitionSpec as P

AXES = ("grp", "row")
MOVE = ("row", "grp")
F32 = jnp.float32
BF16 = jnp.bfloat16
NT = (((1,), (1,)), ((), ()))
VMEM_LIMIT = 56 * 1024 * 1024
LANES = 128
FETCHES = 8


def front_kernel(tables, blocks, groups, cap, me_ref, shard_ref, offset_ref, length_ref, table_ref, out_ref,
                 key_s, off_s, end_s, by_block, meta_v, list_v, held, rows, index_0, index_1, index_2, index_3,
                 table_sem, list_sem, out_sem):
    indices = (index_0, index_1, index_2, index_3)
    look = key_s.shape[0]
    halves = look // LANES
    size = table_ref.shape[1]
    me = me_ref[0]
    part = tables * size // FETCHES
    fetch = []
    for i in range(FETCHES):
        t, at = divmod(i * part, size)
        fetch.append(
            pltpu.make_async_copy(
                table_ref.at[t, pl.ds(at, part)], held.at[pl.ds(i * part, part)], table_sem.at[i]
            )
        )
    early = FETCHES // tables
    for copy in fetch[:early]:
        copy.start()
    later = lax.broadcasted_iota(jnp.int32, (look, look), 0)
    earlier = lax.broadcasted_iota(jnp.int32, (look, look), 1)
    tri = (earlier < later).astype(F32).astype(BF16)
    places = [(lax.broadcasted_iota(jnp.int32, (8, blocks), 0) + 8 * i).astype(F32) for i in range(cap // 8)]
    bags = length_ref.shape[2]
    upto = lax.broadcasted_iota(jnp.int32, (bags, bags), 1) <= lax.broadcasted_iota(jnp.int32, (bags, bags), 0)
    upto = upto.astype(F32).astype(BF16)
    lane = lax.broadcasted_iota(jnp.int32, (blocks, LANES), 1)
    tiles = blocks // groups
    bag_of = []

    def index_copy(t, tile, slot):
        source = list_v.at[pl.ds(t * blocks + tile * groups, groups)]
        return pltpu.make_async_copy(source, indices[slot], list_sem.at[slot])

    for t in range(tables):
        hit = jnp.concatenate(
            [(shard_ref[t, pl.ds(h, blocks, stride=halves), :] == me).astype(F32) for h in range(halves)], axis=1
        )
        rank = lax.dot_general(tri, hit.astype(BF16), NT, preferred_element_type=F32)
        key_s[...] = jnp.where(jnp.transpose(hit) > 0.5, rank, -1.0)
        for h in range(halves):
            off = offset_ref[pl.ds(h * tables + t, blocks, stride=halves * tables), :] + t * size
            packed = off * look + (lane + h * LANES)
            off_s[pl.ds(h * LANES, LANES), :] = jnp.transpose(packed.astype(F32))
        end_s[...] = lax.dot_general(
            upto, length_ref[t].astype(F32).astype(BF16), NT, preferred_element_type=F32
        )

        def step(i, accs):
            for u in range(8):
                key = key_s[pl.ds(i * 8 + u, 1), :]
                off = off_s[pl.ds(i * 8 + u, 1), :]
                accs = tuple(jnp.where(key == pos, off, acc) for acc, pos in zip(accs, places))
            return accs

        found = lax.fori_loop(0, look // 8, step, tuple(jnp.full((8, blocks), -1.0, F32) for _ in places))
        found = [value.astype(jnp.int32) for value in found]
        spots = [(value & (look - 1)).astype(F32) for value in found]

        spare = jnp.full((LANES - cap, blocks), -1.0, F32)
        listed = [(jnp.maximum(value, 0) // look).astype(F32) for value in found]
        by_block[...] = jnp.transpose(jnp.concatenate(listed + [spare], axis=0)).astype(jnp.int32)
        for tile in range(tiles):
            to = pl.ds(t * blocks + tile * groups, groups)
            list_v[to, :] = by_block[pl.ds(tile, groups, stride=tiles), :]
        if t == 0:
            for slot in range(4):
                index_copy(0, slot, slot).start()
            for copy in fetch[early:]:
                copy.start()

        def count(i, accs):
            for u in range(8):
                end = end_s[pl.ds(i * 8 + u, 1), :]
                accs = tuple(acc + jnp.where(end <= spot, 1.0, 0.0) for acc, spot in zip(accs, spots))
            return accs

        counts = lax.fori_loop(0, bags // 8, count, tuple(jnp.zeros((8, blocks), F32) for _ in places))
        bag_of += [jnp.where(value >= 0, number, -1.0) for value, number in zip(found, counts)]
    spare = jnp.full((LANES - tables * cap, blocks), -1.0, F32)
    turned = jnp.transpose(jnp.concatenate(bag_of + [spare], axis=0))
    meta_v[...] = pltpu.roll(turned, lax.rem(me * cap, LANES), 1)
    per_block = tables * cap + 1
    per_tile = groups * per_block
    for tile in range(tiles):
        last_rows = pl.ds(tile * per_tile + per_block - 1, groups, stride=per_block)
        rows[last_rows, :] = meta_v[pl.ds(tile, groups, stride=tiles), :]

    def out_copy(tile):
        span = pl.ds(tile * per_tile, per_tile)
        return pltpu.make_async_copy(rows.at[span], out_ref.at[span], out_sem.at[tile])

    spans = 2
    fours = tiles // 4 // spans
    span_step = 4 * fours
    for span in range(spans):
        for t in range(tables):
            if span == 0:
                for copy in fetch[t * early : (t + 1) * early]:
                    copy.wait()
            last = t == tables - 1

            def four(i, carry):
                for slot in range(4):
                    tile = i * 4 + slot
                    index_copy(t, tile, slot).wait()
                    for u in range(groups):
                        for j in range(cap):
                            row = indices[slot][u, j]
                            at = tile * per_tile + u * per_block + t * cap + j
                            rows[pl.ds(at, 1), :] = held[pl.ds(row, 1), :]
                    if last:
                        out_copy(tile).start()
                    inside = i + 1 < (span + 1) * fours
                    again = span * span_step + slot + (span_step if last else 0)
                    ahead = jnp.where(inside, tile + 4, again)
                    table_ahead = jnp.where(inside, t, (t + 1) % tables)

                    @pl.when(ahead < tiles)
                    def _():
                        index_copy(table_ahead, ahead, slot).start()

                return carry

            lax.fori_loop(span * fours, (span + 1) * fours, four, 0)
    for tile in range(tiles):
        out_copy(tile).wait()


def front(me, shard, offset, lengths, table, blocks, groups, cap):
    tables, size, width = table.shape
    count = blocks * (tables * cap + 1)
    look = shard.shape[1] * LANES // blocks
    return pl.pallas_call(
        functools.partial(front_kernel, tables, blocks, groups, cap),
        out_shape=jax.ShapeDtypeStruct((count, width), F32),
        in_specs=[
            pl.BlockSpec(memory_space=pltpu.SMEM),
            pl.BlockSpec(memory_space=pltpu.VMEM),
            pl.BlockSpec(memory_space=pltpu.VMEM),
            pl.BlockSpec(memory_space=pltpu.VMEM),
            pl.BlockSpec(memory_space=pl.ANY),
        ],
        out_specs=pl.BlockSpec(memory_space=pl.ANY),
        scratch_shapes=[
            pltpu.VMEM((look, blocks), F32),
            pltpu.VMEM((look, blocks), F32),
            pltpu.VMEM((lengths.shape[2], blocks), F32),
            pltpu.VMEM((blocks, LANES), jnp.int32),
            pltpu.VMEM((blocks, LANES), F32),
            pltpu.VMEM((tables * blocks, LANES), jnp.int32),
            pltpu.VMEM((tables * size, width), F32),
            pltpu.VMEM((count, width), F32),
        ]
        + [pltpu.SMEM((groups, LANES), jnp.int32)] * 4
        + [
            pltpu.SemaphoreType.DMA((FETCHES,)),
            pltpu.SemaphoreType.DMA((4,)),
            pltpu.SemaphoreType.DMA((blocks // groups,)),
        ],
        compiler_params=pltpu.CompilerParams(vmem_limit_bytes=VMEM_LIMIT),
        cost_estimate=pl.CostEstimate(flops=60_000_000, bytes_accessed=15_000_000, transcendentals=0),
        name="front",
    )(me, shard, offset, lengths, table)


def pool_kernel(groups, shards, tables, cap, rows_ref, out_ref, out_v, out_sem):
    bags = out_v.shape[1]
    width = rows_ref.shape[1]
    per_block = tables * cap + 1
    step = groups * per_block

    def out_copy(g):
        span = pl.ds(g * tables, tables)
        return pltpu.make_async_copy(out_v.at[span], out_ref.at[span], out_sem.at[g])

    numbers = lax.broadcasted_iota(jnp.int32, (bags, LANES), 0).astype(F32)
    lane = lax.broadcasted_iota(jnp.int32, (1, LANES), 1)

    def group(g, carry):
        start = g * per_block
        meta = rows_ref[pl.ds(start + per_block - 1, shards, stride=step), :]
        for t in range(tables):
            turned = meta if t == 0 else pltpu.roll(meta, LANES - t * cap, 1)
            weight = []
            for v in range(shards * cap // LANES):
                low = v * LANES // cap
                high = ((v + 1) * LANES - 1) // cap
                bag = turned[low : low + 1, :]
                for s in range(low + 1, high + 1):
                    bag = jnp.where(lane >= s * cap - v * LANES, turned[s : s + 1, :], bag)
                weight.append((bag == numbers).astype(F32).astype(BF16))
            rows = jnp.concatenate(
                [rows_ref[pl.ds(start + s * step + t * cap, cap), :] for s in range(shards)], axis=0
            )
            high_part = rows.astype(BF16)
            low_part = (rows - high_part.astype(F32)).astype(BF16)
            both = jnp.dot(
                jnp.concatenate(weight, axis=1),
                jnp.concatenate([high_part, low_part], axis=1),
                preferred_element_type=F32,
            )
            out_v[g * tables + t] = both[:, :width] + both[:, width:]
        out_copy(g).start()
        return carry

    lax.fori_loop(0, groups, group, 0)
    for g in range(groups):
        out_copy(g).wait()


def pool(rows, groups, shards, tables, bags, cap):
    width = rows.shape[1]
    return pl.pallas_call(
        functools.partial(pool_kernel, groups, shards, tables, cap),
        out_shape=jax.ShapeDtypeStruct((groups * tables, bags, width), F32),
        in_specs=[pl.BlockSpec(memory_space=pltpu.VMEM)],
        out_specs=pl.BlockSpec(memory_space=pl.ANY),
        scratch_shapes=[
            pltpu.VMEM((groups * tables, bags, width), F32),
            pltpu.SemaphoreType.DMA((groups,)),
        ],
        compiler_params=pltpu.CompilerParams(vmem_limit_bytes=16 * 1024 * 1024),
        cost_estimate=pl.CostEstimate(flops=20_000_000, bytes_accessed=8_000_000, transcendentals=0),
        name="pool",
    )(rows)


def body(table, row_shard, row_offset, bag_lengths):
    groups = lax.axis_size("grp")
    shards = lax.axis_size("row")
    mine = lax.axis_index("row")
    tables, _, width = table.shape
    blocks, bags = bag_lengths.shape[1:]
    lookups = row_offset.shape[1]
    look = lookups // blocks
    cap = 3 * look // shards

    shard = row_shard.reshape(tables, lookups // LANES, LANES)
    offset = row_offset.reshape(tables, lookups // LANES, LANES).transpose(1, 0, 2)
    offset = offset.reshape(-1, LANES)
    rows = front(mine.reshape(1), shard, offset, bag_lengths, table, blocks, groups, cap)
    moved = lax.all_to_all(rows.reshape(blocks, tables * cap + 1, 1, width), MOVE, 0, 0, tiled=True)
    return pool(moved.reshape(-1, width), groups, shards, tables, bags, cap)


def solution(mesh):
    placed = (P("grp", "row", None), P("grp", None, None), P("grp", None), P("grp", None, None))
    return jax.shard_map(
        body, mesh=mesh, in_specs=placed, out_specs=P(None, AXES, None), check_vma=False
    )
```

```python
import functools

import jax
import jax.numpy as jnp
from jax import lax
from jax.experimental import pallas as pl
from jax.experimental.pallas import tpu as pltpu
from jax.sharding import PartitionSpec as P

AXES = ("grp", "row")
MOVE = ("row", "grp")
F32 = jnp.float32
BF16 = jnp.bfloat16
NT = (((1,), (1,)), ((), ()))
VMEM_LIMIT = 56 * 1024 * 1024
LANES = 128
FETCHES = 8


def front_kernel(tables, blocks, groups, cap, me_ref, shard_ref, offset_ref, length_ref, table_ref, out_ref,
                 key_s, off_s, end_s, by_block, meta_v, list_v, held, rows, index_0, index_1, index_2, index_3,
                 table_sem, list_sem, out_sem):
    indices = (index_0, index_1, index_2, index_3)
    look = key_s.shape[0]
    halves = look // LANES
    size = table_ref.shape[1]
    me = me_ref[0]
    part = tables * size // FETCHES
    fetch = []
    for i in range(FETCHES):
        t, at = divmod(i * part, size)
        fetch.append(
            pltpu.make_async_copy(
                table_ref.at[t, pl.ds(at, part)], held.at[pl.ds(i * part, part)], table_sem.at[i]
            )
        )
    early = FETCHES // tables
    for copy in fetch[:early]:
        copy.start()
    later = lax.broadcasted_iota(jnp.int32, (look, look), 0)
    earlier = lax.broadcasted_iota(jnp.int32, (look, look), 1)
    tri = (earlier < later).astype(F32).astype(BF16)
    places = [(lax.broadcasted_iota(jnp.int32, (8, blocks), 0) + 8 * i).astype(F32) for i in range(cap // 8)]
    bags = length_ref.shape[2]
    upto = lax.broadcasted_iota(jnp.int32, (bags, bags), 1) <= lax.broadcasted_iota(jnp.int32, (bags, bags), 0)
    upto = upto.astype(F32).astype(BF16)
    lane = lax.broadcasted_iota(jnp.int32, (blocks, LANES), 1)
    tiles = blocks // groups
    bag_of = []

    def index_copy(t, tile, slot):
        source = list_v.at[pl.ds(t * blocks + tile * groups, groups)]
        return pltpu.make_async_copy(source, indices[slot], list_sem.at[slot])

    for t in range(tables):
        hit = jnp.concatenate(
            [(shard_ref[t, pl.ds(h, blocks, stride=halves), :] == me).astype(F32) for h in range(halves)], axis=1
        )
        rank = lax.dot_general(tri, hit.astype(BF16), NT, preferred_element_type=F32)
        key_s[...] = jnp.where(jnp.transpose(hit) > 0.5, rank, -1.0)
        for h in range(halves):
            off = offset_ref[pl.ds(h * tables + t, blocks, stride=halves * tables), :] + t * size
            packed = off * look + (lane + h * LANES)
            off_s[pl.ds(h * LANES, LANES), :] = jnp.transpose(packed.astype(F32))
        end_s[...] = lax.dot_general(
            upto, length_ref[t].astype(F32).astype(BF16), NT, preferred_element_type=F32
        )

        def step(i, accs):
            for u in range(8):
                key = key_s[pl.ds(i * 8 + u, 1), :]
                off = off_s[pl.ds(i * 8 + u, 1), :]
                accs = tuple(jnp.where(key == pos, off, acc) for acc, pos in zip(accs, places))
            return accs

        found = lax.fori_loop(0, look // 8, step, tuple(jnp.full((8, blocks), -1.0, F32) for _ in places))
        found = [value.astype(jnp.int32) for value in found]
        spots = [(value & (look - 1)).astype(F32) for value in found]

        spare = jnp.full((LANES - cap, blocks), -1.0, F32)
        listed = [(jnp.maximum(value, 0) // look).astype(F32) for value in found]
        by_block[...] = jnp.transpose(jnp.concatenate(listed + [spare], axis=0)).astype(jnp.int32)
        for tile in range(tiles):
            to = pl.ds(t * blocks + tile * groups, groups)
            list_v[to, :] = by_block[pl.ds(tile, groups, stride=tiles), :]
        if t == 0:
            for slot in range(4):
                index_copy(0, slot, slot).start()
            for copy in fetch[early:]:
                copy.start()

        def count(i, accs):
            for u in range(8):
                end = end_s[pl.ds(i * 8 + u, 1), :]
                accs = tuple(acc + jnp.where(end <= spot, 1.0, 0.0) for acc, spot in zip(accs, spots))
            return accs

        counts = lax.fori_loop(0, bags // 8, count, tuple(jnp.zeros((8, blocks), F32) for _ in places))
        bag_of += [jnp.where(value >= 0, number, -1.0) for value, number in zip(found, counts)]
    spare = jnp.full((LANES - tables * cap, blocks), -1.0, F32)
    turned = jnp.transpose(jnp.concatenate(bag_of + [spare], axis=0))
    meta_v[...] = pltpu.roll(turned, lax.rem(me * cap, LANES), 1)
    per_block = tables * cap + 1
    per_tile = groups * per_block
    for tile in range(tiles):
        last_rows = pl.ds(tile * per_tile + per_block - 1, groups, stride=per_block)
        rows[last_rows, :] = meta_v[pl.ds(tile, groups, stride=tiles), :]

    def out_copy(tile):
        span = pl.ds(tile * per_tile, per_tile)
        return pltpu.make_async_copy(rows.at[span], out_ref.at[span], out_sem.at[tile])

    fours = tiles // 4
    for copy in fetch[:early]:
        copy.wait()

    def four(i, carry):
        t = i // fours
        quad = lax.rem(i, fours)

        @pl.when(i == fours)
        def _():
            for copy in fetch[early:]:
                copy.wait()

        for slot in range(4):
            tile = quad * 4 + slot
            index_copy(t, tile, slot).wait()
            for u in range(groups):
                for j in range(cap):
                    row = indices[slot][u, j]
                    at = tile * per_tile + t * cap + (u * per_block + j)
                    rows[pl.ds(at, 1), :] = held[pl.ds(row, 1), :]

            @pl.when(t == tables - 1)
            def _():
                out_copy(tile).start()

            @pl.when(i + 1 < tables * fours)
            def _():
                index_copy((i + 1) // fours, lax.rem(i + 1, fours) * 4 + slot, slot).start()

        return carry

    lax.fori_loop(0, tables * fours, four, 0)
    for tile in range(tiles):
        out_copy(tile).wait()


def front(me, shard, offset, lengths, table, blocks, groups, cap):
    tables, size, width = table.shape
    count = blocks * (tables * cap + 1)
    look = shard.shape[1] * LANES // blocks
    return pl.pallas_call(
        functools.partial(front_kernel, tables, blocks, groups, cap),
        out_shape=jax.ShapeDtypeStruct((count, width), F32),
        in_specs=[
            pl.BlockSpec(memory_space=pltpu.SMEM),
            pl.BlockSpec(memory_space=pltpu.VMEM),
            pl.BlockSpec(memory_space=pltpu.VMEM),
            pl.BlockSpec(memory_space=pltpu.VMEM),
            pl.BlockSpec(memory_space=pl.ANY),
        ],
        out_specs=pl.BlockSpec(memory_space=pl.ANY),
        scratch_shapes=[
            pltpu.VMEM((look, blocks), F32),
            pltpu.VMEM((look, blocks), F32),
            pltpu.VMEM((lengths.shape[2], blocks), F32),
            pltpu.VMEM((blocks, LANES), jnp.int32),
            pltpu.VMEM((blocks, LANES), F32),
            pltpu.VMEM((tables * blocks, LANES), jnp.int32),
            pltpu.VMEM((tables * size, width), F32),
            pltpu.VMEM((count, width), F32),
        ]
        + [pltpu.SMEM((groups, LANES), jnp.int32)] * 4
        + [
            pltpu.SemaphoreType.DMA((FETCHES,)),
            pltpu.SemaphoreType.DMA((4,)),
            pltpu.SemaphoreType.DMA((blocks // groups,)),
        ],
        compiler_params=pltpu.CompilerParams(vmem_limit_bytes=VMEM_LIMIT),
        cost_estimate=pl.CostEstimate(flops=60_000_000, bytes_accessed=15_000_000, transcendentals=0),
        name="front",
    )(me, shard, offset, lengths, table)


def pool_kernel(groups, shards, tables, cap, rows_ref, out_ref, out_v, out_sem):
    bags = out_v.shape[1]
    width = rows_ref.shape[1]
    per_block = tables * cap + 1
    step = groups * per_block

    def out_copy(g):
        span = pl.ds(g * tables, tables)
        return pltpu.make_async_copy(out_v.at[span], out_ref.at[span], out_sem.at[g])

    numbers = lax.broadcasted_iota(jnp.int32, (bags, LANES), 0).astype(F32)
    lane = lax.broadcasted_iota(jnp.int32, (1, LANES), 1)

    def group(g, carry):
        start = g * per_block
        meta = rows_ref[pl.ds(start + per_block - 1, shards, stride=step), :]
        for t in range(tables):
            turned = meta if t == 0 else pltpu.roll(meta, LANES - t * cap, 1)
            weight = []
            for v in range(shards * cap // LANES):
                low = v * LANES // cap
                high = ((v + 1) * LANES - 1) // cap
                bag = turned[low : low + 1, :]
                for s in range(low + 1, high + 1):
                    bag = jnp.where(lane >= s * cap - v * LANES, turned[s : s + 1, :], bag)
                weight.append((bag == numbers).astype(F32).astype(BF16))
            rows = jnp.concatenate(
                [rows_ref[pl.ds(start + s * step + t * cap, cap), :] for s in range(shards)], axis=0
            )
            high_part = rows.astype(BF16)
            low_part = (rows - high_part.astype(F32)).astype(BF16)
            both = jnp.dot(
                jnp.concatenate(weight, axis=1),
                jnp.concatenate([high_part, low_part], axis=1),
                preferred_element_type=F32,
            )
            out_v[g * tables + t] = both[:, :width] + both[:, width:]
        out_copy(g).start()
        return carry

    lax.fori_loop(0, groups, group, 0)
    for g in range(groups):
        out_copy(g).wait()


def pool(rows, groups, shards, tables, bags, cap):
    width = rows.shape[1]
    return pl.pallas_call(
        functools.partial(pool_kernel, groups, shards, tables, cap),
        out_shape=jax.ShapeDtypeStruct((groups * tables, bags, width), F32),
        in_specs=[pl.BlockSpec(memory_space=pltpu.VMEM)],
        out_specs=pl.BlockSpec(memory_space=pl.ANY),
        scratch_shapes=[
            pltpu.VMEM((groups * tables, bags, width), F32),
            pltpu.SemaphoreType.DMA((groups,)),
        ],
        compiler_params=pltpu.CompilerParams(vmem_limit_bytes=16 * 1024 * 1024),
        cost_estimate=pl.CostEstimate(flops=20_000_000, bytes_accessed=8_000_000, transcendentals=0),
        name="pool",
    )(rows)


def body(table, row_shard, row_offset, bag_lengths):
    groups = lax.axis_size("grp")
    shards = lax.axis_size("row")
    mine = lax.axis_index("row")
    tables, _, width = table.shape
    blocks, bags = bag_lengths.shape[1:]
    lookups = row_offset.shape[1]
    look = lookups // blocks
    cap = 3 * look // shards

    shard = row_shard.reshape(tables, lookups // LANES, LANES)
    offset = row_offset.reshape(tables, lookups // LANES, LANES).transpose(1, 0, 2)
    offset = offset.reshape(-1, LANES)
    rows = front(mine.reshape(1), shard, offset, bag_lengths, table, blocks, groups, cap)
    moved = lax.all_to_all(rows.reshape(blocks, tables * cap + 1, 1, width), MOVE, 0, 0, tiled=True)
    return pool(moved.reshape(-1, width), groups, shards, tables, bags, cap)


def solution(mesh):
    placed = (P("grp", "row", None), P("grp", None, None), P("grp", None), P("grp", None, None))
    return jax.shard_map(
        body, mesh=mesh, in_specs=placed, out_specs=P(None, AXES, None), check_vma=False
    )
```

```python
import functools

import jax
import jax.numpy as jnp
from jax import lax
from jax.experimental import pallas as pl
from jax.experimental.pallas import tpu as pltpu
from jax.sharding import PartitionSpec as P

AXES = ("grp", "row")
MOVE = ("row", "grp")
F32 = jnp.float32
BF16 = jnp.bfloat16
NT = (((1,), (1,)), ((), ()))
VMEM_LIMIT = 56 * 1024 * 1024
LANES = 128
FETCHES = 8


def front_kernel(tables, blocks, groups, cap, me_ref, shard_ref, offset_ref, length_ref, table_ref, out_ref,
                 key_s, off_s, end_s, by_block, meta_v, list_v, held, rows, index_0, index_1, index_2, index_3,
                 table_sem, list_sem, out_sem):
    indices = (index_0, index_1, index_2, index_3)
    look = key_s.shape[0]
    halves = look // LANES
    size = table_ref.shape[1]
    me = me_ref[0]
    part = tables * size // FETCHES
    fetch = []
    for i in range(FETCHES):
        t, at = divmod(i * part, size)
        fetch.append(
            pltpu.make_async_copy(
                table_ref.at[t, pl.ds(at, part)], held.at[pl.ds(i * part, part)], table_sem.at[i]
            )
        )
    early = FETCHES // tables
    for copy in fetch[:early]:
        copy.start()
    later = lax.broadcasted_iota(jnp.int32, (look, look), 0)
    earlier = lax.broadcasted_iota(jnp.int32, (look, look), 1)
    tri = (earlier < later).astype(F32).astype(BF16)
    places = [(lax.broadcasted_iota(jnp.int32, (8, blocks), 0) + 8 * i).astype(F32) for i in range(cap // 8)]
    bags = length_ref.shape[2]
    upto = lax.broadcasted_iota(jnp.int32, (bags, bags), 1) <= lax.broadcasted_iota(jnp.int32, (bags, bags), 0)
    upto = upto.astype(F32).astype(BF16)
    lane = lax.broadcasted_iota(jnp.int32, (blocks, LANES), 1)
    tiles = blocks // groups
    bag_of = []

    def index_copy(t, tile, slot):
        source = list_v.at[pl.ds(t * blocks + tile * groups, groups)]
        return pltpu.make_async_copy(source, indices[slot], list_sem.at[slot])

    for t in range(tables):
        hit = jnp.concatenate(
            [(shard_ref[t, pl.ds(h, blocks, stride=halves), :] == me).astype(F32) for h in range(halves)], axis=1
        )
        rank = lax.dot_general(tri, hit.astype(BF16), NT, preferred_element_type=F32)
        key_s[...] = jnp.where(jnp.transpose(hit) > 0.5, rank, -1.0)
        for h in range(halves):
            off = offset_ref[pl.ds(h * tables + t, blocks, stride=halves * tables), :] + t * size
            packed = off * look + (lane + h * LANES)
            off_s[pl.ds(h * LANES, LANES), :] = jnp.transpose(packed.astype(F32))
        end_s[...] = lax.dot_general(
            upto, length_ref[t].astype(F32).astype(BF16), NT, preferred_element_type=F32
        )

        def step(i, accs):
            for u in range(8):
                key = key_s[pl.ds(i * 8 + u, 1), :]
                off = off_s[pl.ds(i * 8 + u, 1), :]
                accs = tuple(jnp.where(key == pos, off, acc) for acc, pos in zip(accs, places))
            return accs

        found = lax.fori_loop(0, look // 8, step, tuple(jnp.full((8, blocks), -1.0, F32) for _ in places))
        found = [value.astype(jnp.int32) for value in found]
        spots = [(value & (look - 1)).astype(F32) for value in found]

        spare = jnp.full((LANES - cap, blocks), -1.0, F32)
        listed = [(jnp.maximum(value, 0) // look).astype(F32) for value in found]
        by_block[...] = jnp.transpose(jnp.concatenate(listed + [spare], axis=0)).astype(jnp.int32)
        for tile in range(tiles):
            to = pl.ds(t * blocks + tile * groups, groups)
            list_v[to, :] = by_block[pl.ds(tile, groups, stride=tiles), :]
        if t == 0:
            for slot in range(4):
                index_copy(0, slot, slot).start()
            for copy in fetch[early:]:
                copy.start()

        def count(i, accs):
            for u in range(8):
                end = end_s[pl.ds(i * 8 + u, 1), :]
                accs = tuple(acc + jnp.where(end <= spot, 1.0, 0.0) for acc, spot in zip(accs, spots))
            return accs

        counts = lax.fori_loop(0, bags // 8, count, tuple(jnp.zeros((8, blocks), F32) for _ in places))
        bag_of += [jnp.where(value >= 0, number, -1.0) for value, number in zip(found, counts)]
    spare = jnp.full((LANES - tables * cap, blocks), -1.0, F32)
    turned = jnp.transpose(jnp.concatenate(bag_of + [spare], axis=0))
    meta_v[...] = pltpu.roll(turned, lax.rem(me * cap, LANES), 1)
    per_block = tables * cap + 1
    per_tile = groups * per_block
    for tile in range(tiles):
        last_rows = pl.ds(tile * per_tile + per_block - 1, groups, stride=per_block)
        rows[last_rows, :] = meta_v[pl.ds(tile, groups, stride=tiles), :]

    def out_copy(tile):
        span = pl.ds(tile * per_tile, per_tile)
        return pltpu.make_async_copy(rows.at[span], out_ref.at[span], out_sem.at[tile])

    fours = tiles // 4
    for copy in fetch[:early]:
        copy.wait()

    def four(i, carry):
        t = i // fours
        quad = lax.rem(i, fours)

        @pl.when(i == fours)
        def _():
            for copy in fetch[early:]:
                copy.wait()

        for slot in range(4):
            tile = quad * 4 + slot
            index_copy(t, tile, slot).wait()
            for u in range(groups):
                for j in range(cap):
                    row = indices[slot][u, j]
                    at = tile * per_tile + t * cap + (u * per_block + j)
                    rows[pl.ds(at, 1), :] = held[pl.ds(row, 1), :]

            @pl.when(i + 1 < tables * fours)
            def _():
                index_copy((i + 1) // fours, lax.rem(i + 1, fours) * 4 + slot, slot).start()

            @pl.when(t == tables - 1)
            def _():
                out_copy(tile).start()

        return carry

    lax.fori_loop(0, tables * fours, four, 0)
    for tile in range(tiles):
        out_copy(tile).wait()


def front(me, shard, offset, lengths, table, blocks, groups, cap):
    tables, size, width = table.shape
    count = blocks * (tables * cap + 1)
    look = shard.shape[1] * LANES // blocks
    return pl.pallas_call(
        functools.partial(front_kernel, tables, blocks, groups, cap),
        out_shape=jax.ShapeDtypeStruct((count, width), F32),
        in_specs=[
            pl.BlockSpec(memory_space=pltpu.SMEM),
            pl.BlockSpec(memory_space=pltpu.VMEM),
            pl.BlockSpec(memory_space=pltpu.VMEM),
            pl.BlockSpec(memory_space=pltpu.VMEM),
            pl.BlockSpec(memory_space=pl.ANY),
        ],
        out_specs=pl.BlockSpec(memory_space=pl.ANY),
        scratch_shapes=[
            pltpu.VMEM((look, blocks), F32),
            pltpu.VMEM((look, blocks), F32),
            pltpu.VMEM((lengths.shape[2], blocks), F32),
            pltpu.VMEM((blocks, LANES), jnp.int32),
            pltpu.VMEM((blocks, LANES), F32),
            pltpu.VMEM((tables * blocks, LANES), jnp.int32),
            pltpu.VMEM((tables * size, width), F32),
            pltpu.VMEM((count, width), F32),
        ]
        + [pltpu.SMEM((groups, LANES), jnp.int32)] * 4
        + [
            pltpu.SemaphoreType.DMA((FETCHES,)),
            pltpu.SemaphoreType.DMA((4,)),
            pltpu.SemaphoreType.DMA((blocks // groups,)),
        ],
        compiler_params=pltpu.CompilerParams(vmem_limit_bytes=VMEM_LIMIT),
        cost_estimate=pl.CostEstimate(flops=60_000_000, bytes_accessed=15_000_000, transcendentals=0),
        name="front",
    )(me, shard, offset, lengths, table)


def pool_kernel(groups, shards, tables, cap, rows_ref, out_ref, out_v, out_sem):
    bags = out_v.shape[1]
    width = rows_ref.shape[1]
    per_block = tables * cap + 1
    step = groups * per_block

    def out_copy(g):
        span = pl.ds(g * tables, tables)
        return pltpu.make_async_copy(out_v.at[span], out_ref.at[span], out_sem.at[g])

    numbers = lax.broadcasted_iota(jnp.int32, (bags, LANES), 0).astype(F32)
    lane = lax.broadcasted_iota(jnp.int32, (1, LANES), 1)

    def group(g, carry):
        start = g * per_block
        meta = rows_ref[pl.ds(start + per_block - 1, shards, stride=step), :]
        for t in range(tables):
            turned = meta if t == 0 else pltpu.roll(meta, LANES - t * cap, 1)
            weight = []
            for v in range(shards * cap // LANES):
                low = v * LANES // cap
                high = ((v + 1) * LANES - 1) // cap
                bag = turned[low : low + 1, :]
                for s in range(low + 1, high + 1):
                    bag = jnp.where(lane >= s * cap - v * LANES, turned[s : s + 1, :], bag)
                weight.append((bag == numbers).astype(F32).astype(BF16))
            rows = jnp.concatenate(
                [rows_ref[pl.ds(start + s * step + t * cap, cap), :] for s in range(shards)], axis=0
            )
            high_part = rows.astype(BF16)
            low_part = (rows - high_part.astype(F32)).astype(BF16)
            both = jnp.dot(
                jnp.concatenate(weight, axis=1),
                jnp.concatenate([high_part, low_part], axis=1),
                preferred_element_type=F32,
            )
            out_v[g * tables + t] = both[:, :width] + both[:, width:]
        out_copy(g).start()
        return carry

    lax.fori_loop(0, groups, group, 0)
    for g in range(groups):
        out_copy(g).wait()


def pool(rows, groups, shards, tables, bags, cap):
    width = rows.shape[1]
    return pl.pallas_call(
        functools.partial(pool_kernel, groups, shards, tables, cap),
        out_shape=jax.ShapeDtypeStruct((groups * tables, bags, width), F32),
        in_specs=[pl.BlockSpec(memory_space=pltpu.VMEM)],
        out_specs=pl.BlockSpec(memory_space=pl.ANY),
        scratch_shapes=[
            pltpu.VMEM((groups * tables, bags, width), F32),
            pltpu.SemaphoreType.DMA((groups,)),
        ],
        compiler_params=pltpu.CompilerParams(vmem_limit_bytes=16 * 1024 * 1024),
        cost_estimate=pl.CostEstimate(flops=20_000_000, bytes_accessed=8_000_000, transcendentals=0),
        name="pool",
    )(rows)


def body(table, row_shard, row_offset, bag_lengths):
    groups = lax.axis_size("grp")
    shards = lax.axis_size("row")
    mine = lax.axis_index("row")
    tables, _, width = table.shape
    blocks, bags = bag_lengths.shape[1:]
    lookups = row_offset.shape[1]
    look = lookups // blocks
    cap = 3 * look // shards

    shard = row_shard.reshape(tables, lookups // LANES, LANES)
    offset = row_offset.reshape(tables, lookups // LANES, LANES).transpose(1, 0, 2)
    offset = offset.reshape(-1, LANES)
    rows = front(mine.reshape(1), shard, offset, bag_lengths, table, blocks, groups, cap)
    moved = lax.all_to_all(rows.reshape(blocks, tables * cap + 1, 1, width), MOVE, 0, 0, tiled=True)
    return pool(moved.reshape(-1, width), groups, shards, tables, bags, cap)


def solution(mesh):
    placed = (P("grp", "row", None), P("grp", None, None), P("grp", None), P("grp", None, None))
    return jax.shard_map(
        body, mesh=mesh, in_specs=placed, out_specs=P(None, AXES, None), check_vma=False
    )
```
